512 devices in a mesh: clip: 2 (over y), seq: 32 (over z, core), head: 8 (over x).
Axes of the slice: x: 8, y: 2, z: 16, core: 2. Of those that a mesh axis runs over, the one named last changes fastest.
The devices are a block of a 8x8x16 slice.
Arguments:
- queries: bfloat16 [32, 32, 16, 3072], P(('clip', 'head'), 'seq'), parts along dimension 0, may hold values from -15 to 15
- attn_keys: bfloat16 [32, 32, 16, 3072], P(('clip', 'head'), 'seq'), parts along dimension 0, may hold values from -5 to 5
- attn_values: bfloat16 [32, 32, 16, 3072], P(('clip', 'head'), 'seq'), parts along dimension 0, may hold values from -5 to 5
- residual: bfloat16 [32, 32, 16, 5120], P(('clip', 'head'), 'seq'), parts along dimension 0, may hold values from -6 to 6
- out_weight: bfloat16 [3072, 5120], P('head', 'seq'), may hold values from -0.109375 to 0.109375
- out_gate: float32 [5120], replicated, may hold values from 0.3 to 3
- head_shift: float32 [5120], replicated, may hold values from -3 to 3
- head_scale: float32 [5120], replicated, may hold values from -1.5 to 1.5
- head_weight: bfloat16 [5120, 64], replicated, may hold values from -0.078125 to 0.078125
- head_bias: float32 [64], replicated, may hold values from -3 to 3
- conv_weight: bfloat16 [3, 3, 3, 16, 384], replicated, may hold values from -0.3125 to 0.3125
- conv_bias: float32 [384], replicated, may hold values from -3 to 3
- norm_gain: float32 [384], replicated, may hold values from 0.5 to 2
Outputs:
- hidden: bfloat16 [32, 32, 16, 5120], P(('clip', 'head'), 'seq'), parts along dimension 0
- features: bfloat16 [32, 64, 32, 384], P(('clip', 'head'), 'seq'), parts along dimension 0
The draws below stay inside these ranges and needn't reach their ends.
There are 2 independent parts, one for each index of `clip`. The reference program is written for one: setup_inputs(seed, part) draws one part's arguments, and reference() takes and returns one part's arrays. A program takes and returns all parts, laid end to end along the dimension named above; an argument that names none is the same for every part. Nothing has to cross between parts.
All inputs are finite; a program needn't handle non-finite values.
Results may differ from the reference program's by a relative error of at most 0.013.
Values may be sent and summed in bfloat16 or wider, within the bound.
A program may use at most 128 MiB of HBM per device.

```python
import math
import jax
import jax.numpy as jnp
from jax import lax

D = 5120
HEAD_DIM = 128
HEADS = 24
LAT_CH = 16
VAE_CH = 384
WP = 16
F = 16
HP = 32
N_HEAD = 8


def draw_queries(key, part):
    count = F * HP * WP
    values = 3.0 * jnp.clip(jax.random.normal(jax.random.fold_in(key, 11), (count, HEADS, HEAD_DIM), jnp.float32), -5.0, 5.0)
    return values.reshape(F, HP, WP, HEADS * HEAD_DIM).astype(jnp.bfloat16)


def draw_attn_keys(key, part):
    count = F * HP * WP
    values = jnp.clip(jax.random.normal(jax.random.fold_in(key, 12), (count, HEADS, HEAD_DIM), jnp.float32), -5.0, 5.0)
    return values.reshape(F, HP, WP, HEADS * HEAD_DIM).astype(jnp.bfloat16)


def block_levels(own_key, dims, shards, low, top_value):
    def one(dim, shards_of):
        heights = jax.random.uniform(jax.random.fold_in(jax.random.fold_in(own_key, 6), dim), (shards_of,), jnp.float32, low / len(shards), top_value / len(shards))
        return jnp.repeat(jnp.exp(heights), dims[dim] // shards_of).reshape((-1,) + (1,) * (len(dims) - dim - 1))

    loudness = one(*shards[0])
    for cut in shards[1:]:
        loudness = loudness * one(*cut)
    return loudness


def centred(own_key, shape, deviation, reach, split=(), held_as=jnp.bfloat16):
    level = block_levels(own_key, shape, split, -0.22, 0.18) if split else 1.0
    entries = jax.random.normal(own_key, shape, jnp.float32) * deviation * level
    return jnp.minimum(jnp.maximum(entries, -reach), reach).astype(held_as)


def setup_inputs(seed: int = 0, part: int = 0) -> dict:
    key_list = jax.random.split(jax.random.key(seed), 14)
    own_keys = jax.random.split(jax.random.fold_in(key_list[13], part), 14)
    queries = draw_queries(jax.random.fold_in(jax.random.fold_in(key_list[13], part), 71), part)
    attn_keys = draw_attn_keys(jax.random.fold_in(jax.random.fold_in(key_list[13], part), 71), part)
    attn_values = centred(own_keys[2], (F, HP, WP, HEADS * HEAD_DIM), 1.0, 5.0, ((0, 8), (1, 32)))
    residual = centred(own_keys[3], (F, HP, WP, D), 1.0, 6.0, ((0, 8), (1, 32)))
    out_weight = centred(key_list[4], (HEADS * HEAD_DIM, D), (HEADS * HEAD_DIM) ** -0.5, 0.109375, ((0, 8), (1, 32)))
    out_gate = jnp.clip(jnp.exp(jax.random.uniform(key_list[5], (D,), jnp.float32, math.log(0.3), math.log(3.0))), 0.3, 3.0)
    head_shift = centred(key_list[6], (D,), 0.5, 3.0, (), jnp.float32)
    head_scale = centred(key_list[7], (D,), 0.3, 1.5, (), jnp.float32)
    head_weight = centred(key_list[8], (D, 4 * LAT_CH), D ** -0.5, 0.078125)
    head_bias = centred(key_list[9], (4 * LAT_CH,), 0.5, 3.0, (), jnp.float32)
    conv_weight = centred(key_list[10], (3, 3, 3, LAT_CH, VAE_CH), (27 * LAT_CH) ** -0.5, 0.3125)
    conv_bias = centred(key_list[11], (VAE_CH,), 0.5, 3.0, (), jnp.float32)
    norm_gain = jnp.clip(jnp.exp(jax.random.uniform(key_list[12], (VAE_CH,), jnp.float32, math.log(0.5), math.log(2.0))), 0.5, 2.0)
    return {"queries": queries, "attn_keys": attn_keys, "attn_values": attn_values, "residual": residual, "out_weight": out_weight, "out_gate": out_gate, "head_shift": head_shift, "head_scale": head_scale, "head_weight": head_weight, "head_bias": head_bias, "conv_weight": conv_weight, "conv_bias": conv_bias, "norm_gain": norm_gain}


def head_latent(hidden, head_shift, head_scale, head_weight, head_bias):
    values = hidden.astype(jnp.float32)
    center = values - lax.optimization_barrier(jnp.mean(values, -1, keepdims=True))
    spread = lax.optimization_barrier(jnp.mean(center * center, -1, keepdims=True))
    normed = (center * lax.rsqrt(spread + 1e-06) * (1.0 + head_scale) + head_shift).astype(jnp.bfloat16)
    flat = normed.reshape(-1, normed.shape[-1])
    latent = (jnp.dot(flat, head_weight, preferred_element_type=jnp.float32) + head_bias).astype(jnp.bfloat16)
    frames, height, breadth = (hidden.shape[0], hidden.shape[1], hidden.shape[2])
    channels = head_weight.shape[1] // 4
    patches = latent.reshape(frames, height, breadth, 2, 2, channels).transpose(0, 1, 3, 2, 4, 5)
    return patches.reshape(frames, height * 2, breadth * 2, channels)

def convolve(padded, frames, conv_weight, conv_bias, norm_gain):
    height = padded.shape[1] - 2
    breadth = padded.shape[2] - 2
    stacked = jnp.concatenate([padded[time_off:time_off + frames, row_off:row_off + height, col_off:col_off + breadth] for time_off in range(3) for row_off in range(3) for col_off in range(3)], -1)
    kernel = conv_weight.reshape(-1, conv_weight.shape[-1])
    linear = jnp.dot(stacked.reshape(-1, stacked.shape[-1]), kernel, preferred_element_type=jnp.float32) + conv_bias
    normed = linear * lax.rsqrt(lax.optimization_barrier(jnp.mean(linear * linear, -1, keepdims=True)) + 1e-06) * norm_gain
    return jax.nn.silu(normed).astype(jnp.bfloat16).reshape(frames, height, breadth, -1)

def one_head(triple):
    query_one, key_one, value_one = triple
    scores = jnp.dot(query_one, key_one.T, preferred_element_type=jnp.float32) * query_one.shape[-1] ** (-0.5)
    peak = lax.optimization_barrier(jnp.max(scores, -1, keepdims=True))
    weights = jnp.exp(scores - peak)
    denominator = lax.optimization_barrier(jnp.sum(weights, -1, keepdims=True))
    product = jnp.dot(weights.astype(jnp.bfloat16), value_one, preferred_element_type=jnp.float32)
    return (product / denominator).astype(jnp.bfloat16)

def add_group(running_sum, pair):
    term = jnp.dot(pair[0], pair[1], preferred_element_type=jnp.float32).astype(jnp.bfloat16)
    term = lax.optimization_barrier(term).astype(jnp.float32)
    return (running_sum + term, None)

def reference(queries, attn_keys, attn_values, residual, out_weight, out_gate, head_shift, head_scale, head_weight, head_bias, conv_weight, conv_bias, norm_gain):
    count = F * HP * WP
    query_heads = queries.reshape(count, HEADS, HEAD_DIM).transpose(1, 0, 2)
    key_heads = attn_keys.reshape(count, HEADS, HEAD_DIM).transpose(1, 0, 2)
    value_heads = attn_values.reshape(count, HEADS, HEAD_DIM).transpose(1, 0, 2)
    attended = lax.map(one_head, (query_heads, key_heads, value_heads))
    attended = attended.transpose(1, 0, 2).reshape(count, HEADS * HEAD_DIM)
    group_width = HEADS // N_HEAD * HEAD_DIM
    groups_in = attended.reshape(count, N_HEAD, group_width).transpose(1, 0, 2)
    weights_in = out_weight.reshape(N_HEAD, group_width, D)
    projected, _ = lax.scan(add_group, jnp.zeros((count, D), jnp.float32), (groups_in, weights_in))
    projected = projected.reshape(F, HP, WP, D)
    hidden = (residual.astype(jnp.float32) + out_gate * projected).astype(jnp.bfloat16)
    video = head_latent(hidden, head_shift, head_scale, head_weight, head_bias)
    padded = jnp.pad(video, ((2, 0), (1, 1), (1, 1), (0, 0)))
    features = convolve(padded, F, conv_weight, conv_bias, norm_gain)
    return (hidden, features)
```

```python
import functools

import jax
import jax.numpy as jnp
from jax import lax
from jax.experimental import pallas as pl
from jax.experimental.pallas import tpu as pltpu
from jax.sharding import PartitionSpec as P

HEAD_DIM = 128


def from_behind(value, axis, steps):
    count = lax.axis_size(axis)
    first, last = (max(0, -steps), min(count, count - steps))
    return lax.ppermute(value, axis, [(source, source + steps) for source in range(first, last)])


def padded_2(x, sides, width):
    for axis, dim in sides:
        peers, length = (lax.axis_size(axis), x.shape[dim])
        up = [(i, (i + 1) % peers) for i in range(peers - 1)]
        down = [(j, i) for i, j in up]
        last = lax.slice_in_dim(x, length - width, length, axis=dim)
        first = lax.slice_in_dim(x, 0, width, axis=dim)
        before = lax.ppermute(last, axis, up)
        after = lax.ppermute(first, axis, down)
        x = jnp.concatenate([before, x, after], axis=dim)
    return x


def head_latent(hidden, head_shift, head_scale, head_weight, head_bias):
    values = hidden.astype(jnp.float32)
    center = values - jnp.mean(values, -1, keepdims=True)
    spread = jnp.mean(center * center, -1, keepdims=True)
    normed = (center * lax.rsqrt(spread + 1e-06) * (1.0 + head_scale) + head_shift).astype(
        jnp.bfloat16
    )
    flat = normed.reshape(-1, normed.shape[-1])
    latent = (jnp.dot(flat, head_weight, preferred_element_type=jnp.float32) + head_bias).astype(
        jnp.bfloat16
    )
    frames, height, breadth = (hidden.shape[0], hidden.shape[1], hidden.shape[2])
    channels = head_weight.shape[1] // 4
    patches = latent.reshape(frames, height, breadth, 2, 2, channels).transpose(0, 1, 3, 2, 4, 5)
    return patches.reshape(frames, height * 2, breadth * 2, channels)


def convolve(padded, frames, conv_weight, conv_bias, norm_gain):
    height = padded.shape[1] - 2
    breadth = padded.shape[2] - 2
    stacked = jnp.concatenate(
        [
            padded[
                time_off : time_off + frames,
                row_off : row_off + height,
                col_off : col_off + breadth,
            ]
            for time_off in range(3)
            for row_off in range(3)
            for col_off in range(3)
        ],
        -1,
    )
    kernel = conv_weight.reshape(-1, conv_weight.shape[-1])
    linear = (
        jnp.dot(stacked.reshape(-1, stacked.shape[-1]), kernel, preferred_element_type=jnp.float32)
        + conv_bias
    )
    normed = linear * lax.rsqrt(jnp.mean(linear * linear, -1, keepdims=True) + 1e-06) * norm_gain
    return jax.nn.silu(normed).astype(jnp.bfloat16).reshape(frames, height, breadth, -1)


MESH = pl.DeviceIdType.MESH


def attend_kernel(nx, nz, q_in, k_in, v_in, out_ref, qbuf, kbuf, vbuf, qt, acc, stat,
                  a2a_send, a2a_recv, ring_send, ring_recv, pair_send, pair_recv):
    x = lax.axis_index("head")
    s = lax.axis_index("seq")
    z, c = s // 2, lax.rem(s, 2)
    rows, width = k_in.shape[0], kbuf.shape[3]
    heads = width // HEAD_DIM
    scale = HEAD_DIM ** (-0.5)
    half = nz // 2

    def seq_of(zz, cc):
        return lax.rem(zz + 2 * nz, nz) * 2 + cc

    barrier = pltpu.get_barrier_semaphore()
    for d in range(1, nx):
        pl.semaphore_signal(barrier, inc=1, device_id={"head": lax.rem(x + d, nx)}, device_id_type=MESH)
    for other in (seq_of(z + 1, c), seq_of(z - 1, c), seq_of(z, 1 - c)):
        pl.semaphore_signal(barrier, inc=1, device_id={"seq": other}, device_id_type=MESH)
    pl.semaphore_wait(barrier, nx + 2)

    ins = (k_in, v_in, q_in)
    mine = (kbuf.at[c, z], vbuf.at[c, z], qbuf)
    own_rows = pl.ds(pl.multiple_of(x * rows, rows), rows)
    own_cols = pl.ds(pl.multiple_of(x * width, width), width)
    for i in range(3):
        for d in range(1, nx):
            peer = lax.rem(x + (d + 1) // 2 if d % 2 else x + nx - d // 2, nx)
            cols = pl.ds(pl.multiple_of(peer * width, width), width)
            pltpu.make_async_remote_copy(
                src_ref=ins[i].at[:, cols], dst_ref=mine[i].at[own_rows, :],
                send_sem=a2a_send.at[i], recv_sem=a2a_recv.at[i],
                device_id={"head": peer}, device_id_type=MESH).start()
    for i in range(3):
        mine[i][own_rows, :] = ins[i][:, own_cols]

    def all_but_one(i):
        part = mine[i].at[pl.ds(0, rows * (nx - 1)), :]
        return pltpu.make_async_remote_copy(
            src_ref=part, dst_ref=part, send_sem=a2a_send.at[i], recv_sem=a2a_recv.at[i],
            device_id={"head": lax.rem(x + 1, nx)}, device_id_type=MESH)

    bufs = (kbuf, vbuf)

    def hop(kv, direction, step):
        slot = bufs[kv].at[c, lax.rem(z - direction * (step - 1) + nz, nz)]
        flow = 2 * kv + (1 if direction > 0 else 0)
        return pltpu.make_async_remote_copy(
            src_ref=slot, dst_ref=slot, send_sem=ring_send.at[flow, step], recv_sem=ring_recv.at[flow, step],
            device_id={"seq": seq_of(z + direction, c)}, device_id_type=MESH)

    def landed(kv, direction, step):
        slot = bufs[kv].at[c, lax.rem(z - direction * step + nz, nz)]
        flow = 2 * kv + (1 if direction > 0 else 0)
        return pltpu.make_async_remote_copy(
            src_ref=slot, dst_ref=slot, send_sem=ring_send.at[flow, step], recv_sem=ring_recv.at[flow, step],
            device_id={"seq": seq_of(z + direction, c)}, device_id_type=MESH)

    def share(kv, zz):
        slot = bufs[kv].at[c, zz]
        return pltpu.make_async_remote_copy(
            src_ref=slot, dst_ref=slot, send_sem=pair_send.at[kv, zz], recv_sem=pair_recv.at[kv, zz],
            device_id={"seq": seq_of(z, 1 - c)}, device_id_type=MESH)

    def shared(kv, zz):
        slot = bufs[kv].at[1 - c, zz]
        return pltpu.make_async_remote_copy(
            src_ref=slot, dst_ref=slot, send_sem=pair_send.at[kv, zz], recv_sem=pair_recv.at[kv, zz],
            device_id={"seq": seq_of(z, 1 - c)}, device_id_type=MESH)

    for kv in range(2):
        all_but_one(kv).wait_recv()
        for direction in (1, -1):
            hop(kv, direction, 1).start()
        share(kv, z).start()
    all_but_one(2).wait_recv()

    for j in range(heads):
        qt[j] = qbuf[:, j * HEAD_DIM:(j + 1) * HEAD_DIM].astype(jnp.float32).T.astype(jnp.bfloat16)
    acc[...] = jnp.zeros_like(acc)
    stat[:, 0] = jnp.full(stat[:, 0].shape, -1e30, jnp.float32)
    stat[:, 1] = jnp.zeros_like(stat[:, 1])

    def attend(lane, zz):
        for j in range(heads):
            cols = pl.ds(j * HEAD_DIM, HEAD_DIM)
            scores = lax.dot_general(kbuf[lane, zz, :, cols], qt[j], (((1,), (0,)), ((), ())),
                                     preferred_element_type=jnp.float32)
            before = stat[j, 0]
            peak = jnp.maximum(before, jnp.max(scores, 0, keepdims=True))
            factor = jnp.exp((before - peak) * scale)
            weights = jnp.exp((scores - peak) * scale)
            stat[j, 1] = stat[j, 1] * factor + jnp.sum(weights, 0, keepdims=True)
            stat[j, 0] = peak
            acc[j] = acc[j] * factor + lax.dot_general(
                vbuf[lane, zz, :, cols], weights.astype(jnp.bfloat16), (((0,), (0,)), ((), ())),
                preferred_element_type=jnp.float32)

    def last_hop(kv, direction):
        return half if (kv == 0) == (direction > 0) else half - 1

    attend(c, z)
    for kv in range(2):
        shared(kv, z).wait_recv()
    attend(1 - c, z)

    def step(h, carry):
        for kv in range(2):
            for direction in (1, -1):
                landed(kv, direction, h).wait_recv()

                @pl.when(h < last_hop(kv, direction))
                def _():
                    hop(kv, direction, h + 1).start()

                share(kv, lax.rem(z - direction * h + nz, nz)).start()

        def block(i, carry):
            zz = lax.rem(z - (1 - 2 * i) * h + nz, nz)
            attend(c, zz)
            for kv in range(2):
                shared(kv, zz).wait_recv()
            attend(1 - c, zz)
            return carry

        lax.fori_loop(0, 2, block, 0)
        return carry

    lax.fori_loop(1, half, step, 0)
    far = lax.rem(z + half, nz)
    for kv in range(2):
        landed(kv, 1 if kv == 0 else -1, half).wait_recv()
        share(kv, far).start()
    attend(c, far)
    for kv in range(2):
        shared(kv, far).wait_recv()
    attend(1 - c, far)

    for j in range(heads):
        whole = acc[j] / stat[j, 1]
        out_ref[:, j * HEAD_DIM:(j + 1) * HEAD_DIM] = whole.T.astype(out_ref.dtype)

    for i in range(3):
        all_but_one(i).wait_send()

    def drain(h, carry):
        for kv in range(2):
            for direction in (1, -1):
                @pl.when(h <= last_hop(kv, direction))
                def _():
                    hop(kv, direction, h).wait_send()
        return carry

    lax.fori_loop(1, half + 1, drain, 0)

    def drain_pair(zz, carry):
        for kv in range(2):
            share(kv, zz).wait_send()
        return carry

    lax.fori_loop(0, nz, drain_pair, 0)


def attention(queries, attn_keys, attn_values):
    nx, nz = lax.axis_size("head"), lax.axis_size("seq") // 2
    frames, height, breadth, features = queries.shape
    rows, width = frames * height * breadth, features // nx
    heads = width // HEAD_DIM
    count = rows * nx
    flat = [a.reshape(rows, features) for a in (queries, attn_keys, attn_values)]
    kept = pl.BlockSpec(memory_space=pltpu.VMEM)
    dma = pltpu.SemaphoreType.DMA
    return pl.pallas_call(
        functools.partial(attend_kernel, nx, nz),
        out_shape=jax.ShapeDtypeStruct((count, width), jnp.bfloat16),
        in_specs=[kept] * 3,
        out_specs=kept,
        scratch_shapes=[
            pltpu.VMEM((count, width), jnp.bfloat16),
            pltpu.VMEM((2, nz, count, width), jnp.bfloat16),
            pltpu.VMEM((2, nz, count, width), jnp.bfloat16),
            pltpu.VMEM((heads, HEAD_DIM, count), jnp.bfloat16),
            pltpu.VMEM((heads, HEAD_DIM, count), jnp.float32),
            pltpu.VMEM((heads, 2, 1, count), jnp.float32),
            dma((3,)), dma((3,)),
            dma((4, nz // 2 + 1)), dma((4, nz // 2 + 1)),
            dma((2, nz)), dma((2, nz)),
        ],
        compiler_params=pltpu.CompilerParams(
            collective_id=0, has_side_effects=True, vmem_limit_bytes=40 * 2**20),
        cost_estimate=pl.CostEstimate(flops=4 * count * count * 2 * nz * width, bytes_accessed=2**21, transcendentals=0),
        name="attention_ring",
    )(*flat)


def on_device(
    queries,
    attn_keys,
    attn_values,
    residual,
    out_weight,
    out_gate,
    head_shift,
    head_scale,
    head_weight,
    head_bias,
    conv_weight,
    conv_bias,
    norm_gain,
):
    frames_dev, height, breadth = queries.shape[:3]
    frames_all = frames_dev * lax.axis_size("head")
    attended = attention(queries, attn_keys, attn_values)
    partial_value = jnp.dot(
        attended,
        lax.all_gather(out_weight, "seq", axis=1, tiled=True),
        preferred_element_type=jnp.float32,
    )
    partial_value = partial_value.reshape(frames_all, height, breadth, partial_value.shape[-1])
    owned = lax.psum_scatter(
        partial_value.astype(jnp.bfloat16), "head", scatter_dimension=0, tiled=True
    ).astype(jnp.float32)
    hidden = (residual.astype(jnp.float32) + out_gate * owned).astype(jnp.bfloat16)
    own_video = head_latent(hidden, head_shift, head_scale, head_weight, head_bias)
    earlier = from_behind(own_video, "head", 1)
    video = jnp.concatenate([earlier, own_video], 0)
    extended = padded_2(video, (("seq", 1),), 1)
    padded = jnp.pad(extended, ((0, 0), (0, 0), (1, 1), (0, 0)))
    features = convolve(padded, frames_dev, conv_weight, conv_bias, norm_gain)
    return (hidden, features)


def solution(mesh):
    return jax.shard_map(
        on_device,
        mesh=mesh,
        in_specs=(
            P(("clip", "head"), "seq", None, None),
            P(("clip", "head"), "seq", None, None),
            P(("clip", "head"), "seq", None, None),
            P(("clip", "head"), "seq", None, None),
            P("head", "seq"),
            P(),
            P(),
            P(),
            P(),
            P(),
            P(),
            P(),
            P(),
        ),
        out_specs=(P(("clip", "head"), "seq", None, None), P(("clip", "head"), "seq", None, None)),
        check_vma=False,
    )
```

```python
import functools

import jax
import jax.numpy as jnp
from jax import lax
from jax.experimental import pallas as pl
from jax.experimental.pallas import tpu as pltpu
from jax.sharding import PartitionSpec as P

HEAD_DIM = 128
MESH = pl.DeviceIdType.MESH
SUBS = 2


def convolve(padded, frames, conv_weight, conv_bias, norm_gain):
    height = padded.shape[1] - 2
    breadth = padded.shape[2] - 2
    stacked = jnp.concatenate(
        [
            padded[
                time_off : time_off + frames,
                row_off : row_off + height,
                col_off : col_off + breadth,
            ]
            for time_off in range(3)
            for row_off in range(3)
            for col_off in range(3)
        ],
        -1,
    )
    kernel = conv_weight.reshape(-1, conv_weight.shape[-1])
    linear = (
        jnp.dot(stacked.reshape(-1, stacked.shape[-1]), kernel, preferred_element_type=jnp.float32)
        + conv_bias
    )
    normed = linear * lax.rsqrt(jnp.mean(linear * linear, -1, keepdims=True) + 1e-06) * norm_gain
    return jax.nn.silu(normed).astype(jnp.bfloat16).reshape(frames, height, breadth, -1)


def block_kernel(nx, nz, q_in, k_in, v_in, w_in, res_in, gate_in, shift_in, scale_in, hw_in, hb_in,
                 hidden_ref, lat_ref,
                 qbuf, kbuf, vbuf, wbuf, qt, acc, stat, part, sums_out, sums_in, tokens, owned, lat,
                 res, gate, shift, gain, hw, hb,
                 local_sem, a2a_send, a2a_recv, ring_send, ring_recv, pair_send, pair_recv,
                 w_send, w_recv, wpair_send, wpair_recv, rs_send, rs_recv, halo_send, halo_recv, out_sem):
    x = lax.axis_index("head")
    s = lax.axis_index("seq")
    z, c = s // 2, lax.rem(s, 2)
    nseq = 2 * nz
    rows, width = k_in.shape[0], kbuf.shape[3]
    heads = width // HEAD_DIM
    scale = HEAD_DIM ** (-0.5)
    half = nz // 2
    features = part.shape[1]

    def seq_of(zz, cc):
        return lax.rem(zz + 2 * nz, nz) * 2 + cc

    def remote(src, dst, send, recv, **where):
        return pltpu.make_async_remote_copy(
            src_ref=src, dst_ref=dst, send_sem=send, recv_sem=recv, device_id=where, device_id_type=MESH)

    own_rows = pl.ds(pl.multiple_of(x * rows, rows), rows)
    own_cols = pl.ds(pl.multiple_of(x * width, width), width)
    mine = (kbuf.at[c, z], vbuf.at[c, z], qbuf)
    ins = (k_in, v_in, q_in)
    loads = [pltpu.make_async_copy(ins[i].at[:, own_cols], mine[i].at[own_rows, :], local_sem.at[i]) for i in range(3)]
    loads.append(pltpu.make_async_copy(w_in, wbuf.at[z, c], local_sem.at[3]))
    late = ((res_in, res), (gate_in, gate), (shift_in, shift), (scale_in, gain), (hw_in, hw), (hb_in, hb))
    loads += [pltpu.make_async_copy(a, b, local_sem.at[4 + i]) for i, (a, b) in enumerate(late)]
    for load in loads:
        load.start()

    def away(value, by, size):
        return lax.rem(value + by + size, size)

    lat[...] = jnp.zeros_like(lat)
    barrier = pltpu.get_barrier_semaphore()
    for d in range(1, nx):
        pl.semaphore_signal(barrier, inc=1, device_id={"head": away(x, d, nx)}, device_id_type=MESH)
    for other in (seq_of(z + 1, c), seq_of(z - 1, c), seq_of(z, 1 - c), away(s, 2 * c - 1, nseq)):
        pl.semaphore_signal(barrier, inc=1, device_id={"seq": other}, device_id_type=MESH)
    for dx in (1, -1):
        for ds in (1, -1):
            pl.semaphore_signal(barrier, inc=1, device_id={"head": away(x, dx, nx), "seq": away(s, ds, nseq)},
                                device_id_type=MESH)
    pl.semaphore_wait(barrier, nx + 7)

    for i in range(3):
        for d in range(1, nx):
            peer = lax.rem(x + (d + 1) // 2 if d % 2 else x + nx - d // 2, nx)
            cols = pl.ds(pl.multiple_of(peer * width, width), width)
            remote(ins[i].at[:, cols], mine[i].at[own_rows, :], a2a_send.at[i], a2a_recv.at[i], head=peer).start()

    def all_but_one(i):
        piece = mine[i].at[pl.ds(0, rows * (nx - 1)), :]
        return remote(piece, piece, a2a_send.at[i], a2a_recv.at[i], head=away(x, 1, nx))

    bufs = (kbuf, vbuf)

    def hop(kv, direction, step, back):
        slot = bufs[kv].at[c, lax.rem(z - direction * back + 2 * nz, nz)]
        flow = 2 * kv + (1 if direction > 0 else 0)
        return remote(slot, slot, ring_send.at[flow, step], ring_recv.at[flow, step], seq=seq_of(z + direction, c))

    def w_hop(direction, step, back):
        slot = wbuf.at[lax.rem(z - direction * back + 2 * nz, nz), c]
        flow = 1 if direction > 0 else 0
        return remote(slot, slot, w_send.at[flow, step], w_recv.at[flow, step], seq=seq_of(z + direction, c))

    def share(kv, zz, cc):
        slot = bufs[kv].at[cc, zz]
        return remote(slot, slot, pair_send.at[kv, zz], pair_recv.at[kv, zz], seq=seq_of(z, 1 - c))

    def w_share(zz, cc):
        slot = wbuf.at[zz, cc]
        return remote(slot, slot, wpair_send.at[zz], wpair_recv.at[zz], seq=seq_of(z, 1 - c))

    loads[3].wait()
    for direction in (1, -1):
        w_hop(direction, 1, 0).start()
    w_share(z, c).start()
    for kv in range(2):
        loads[kv].wait()
        all_but_one(kv).wait_recv()
        for direction in (1, -1):
            hop(kv, direction, 1, 0).start()
        share(kv, z, c).start()
    loads[2].wait()
    all_but_one(2).wait_recv()

    for j in range(heads):
        qt[j] = qbuf[:, j * HEAD_DIM:(j + 1) * HEAD_DIM].astype(jnp.float32).T.astype(jnp.bfloat16)
    acc[...] = jnp.zeros_like(acc)
    stat[:, 0] = jnp.full(stat[:, 0].shape, -1e30, jnp.float32)
    stat[:, 1] = jnp.zeros_like(stat[:, 1])

    def attend(lane, zz):
        for j in range(heads):
            cols = pl.ds(j * HEAD_DIM, HEAD_DIM)
            scores = lax.dot_general(kbuf[lane, zz, :, cols], qt[j], (((1,), (0,)), ((), ())),
                                     preferred_element_type=jnp.float32)
            before = stat[j, 0]
            peak = jnp.maximum(before, jnp.max(scores, 0, keepdims=True))
            factor = jnp.exp((before - peak) * scale)
            weights = jnp.exp((scores - peak) * scale)
            stat[j, 1] = stat[j, 1] * factor + jnp.sum(weights, 0, keepdims=True)
            stat[j, 0] = peak
            acc[j] = acc[j] * factor + lax.dot_general(
                vbuf[lane, zz, :, cols], weights.astype(jnp.bfloat16), (((0,), (0,)), ((), ())),
                preferred_element_type=jnp.float32)

    def last_hop(kv, direction):
        return half if (kv == 0) == (direction > 0) else half - 1

    def w_last(direction):
        return half if direction > 0 else half - 1

    def both_lanes(zz):
        attend(c, zz)
        for kv in range(2):
            share(kv, zz, 1 - c).wait_recv()
        attend(1 - c, zz)

    both_lanes(z)

    def step(h, carry):
        for kv in range(2):
            for direction in (1, -1):
                hop(kv, direction, h, h).wait_recv()

                @pl.when(h < last_hop(kv, direction))
                def _():
                    hop(kv, direction, h + 1, h).start()

                share(kv, lax.rem(z - direction * h + nz, nz), c).start()
        for direction in (1, -1):
            w_hop(direction, h, h).wait_recv()

            @pl.when(h < w_last(direction))
            def _():
                w_hop(direction, h + 1, h).start()

            w_share(lax.rem(z - direction * h + nz, nz), c).start()

        def block(i, carry):
            both_lanes(lax.rem(z - (1 - 2 * i) * h + nz, nz))
            return carry

        lax.fori_loop(0, 2, block, 0)
        return carry

    lax.fori_loop(1, half, step, 0)
    far = lax.rem(z + half, nz)
    for kv in range(2):
        hop(kv, 1 if kv == 0 else -1, half, half).wait_recv()
        share(kv, far, c).start()
    w_hop(1, half, half).wait_recv()
    w_share(far, c).start()
    both_lanes(far)

    for j in range(heads):
        tokens[:, j * HEAD_DIM:(j + 1) * HEAD_DIM] = (acc[j] / stat[j, 1]).T.astype(jnp.bfloat16)

    def w_land(zz, carry):
        w_share(zz, 1 - c).wait_recv()
        return carry

    lax.fori_loop(0, nz, w_land, 0)

    w_rows = w_in.shape[0]
    tile = 4 * w_rows

    def project(i, carry):
        columns = wbuf[pl.ds(2 * i, 2)].reshape(tile, width)
        part[:, pl.ds(pl.multiple_of(i * tile, tile), tile)] = lax.dot_general(
            tokens[...], columns, (((1,), (1,)), ((), ())), preferred_element_type=jnp.float32)
        return carry

    lax.fori_loop(0, nz // 2, project, 0)
    block = features // (2 * SUBS)

    def term(flow, direction, t):
        owner = lax.rem(x - direction * t + 2 * nx, nx)
        return part[pl.ds(pl.multiple_of(owner * rows, rows), rows), flow * block:(flow + 1) * block]

    def rs(flow, direction, t):
        return remote(sums_out.at[flow, t], sums_in.at[flow, t], rs_send.at[flow, t], rs_recv.at[flow, t],
                      head=away(x, direction, nx))

    flows = [(f, 1 if f % 2 else -1) for f in range(2 * SUBS)]
    for f, direction in flows:
        sums_out[f, 1] = term(f, direction, 1).astype(jnp.bfloat16)
    for f, direction in flows:
        rs(f, direction, 1).start()

    def rs_step(t, carry):
        for f, direction in flows:
            rs(f, direction, t - 1).wait_recv()
            sums_out[f, t] = (sums_in[f, t - 1].astype(jnp.float32) + term(f, direction, t)).astype(jnp.bfloat16)
            rs(f, direction, t).start()
        return carry

    lax.fori_loop(2, nx, rs_step, 0)
    for load in loads[4:]:
        load.wait()
    for f, direction in flows:
        rs(f, direction, nx - 1).wait_recv()
        cols = slice(f * block, (f + 1) * block)
        total = sums_in[f, nx - 1].astype(jnp.float32) + term(f, direction, nx)
        owned[:, cols] = (res[:, cols].astype(jnp.float32) + gate[:, cols] * total).astype(jnp.bfloat16)

    out = pltpu.make_async_copy(owned, hidden_ref, out_sem.at[0])
    out.start()
    values = owned[...].astype(jnp.float32)
    center = values - jnp.mean(values, -1, keepdims=True)
    spread = jnp.mean(center * center, -1, keepdims=True)
    normed = (center * lax.rsqrt(spread + 1e-06) * (1.0 + gain[...]) + shift[...]).astype(jnp.bfloat16)
    latent = jnp.dot(normed, hw[...], preferred_element_type=jnp.float32) + hb[...]
    cells = latent.shape[1]
    lat[1, 1, :, 0:cells] = latent.astype(jnp.bfloat16)

    sends = []
    for i, (dx, ds) in enumerate(((0, 1), (0, -1), (1, 0), (1, 1), (1, -1))):
        def copy(i=i, dx=dx, ds=ds):
            return remote(lat.at[1, 1], lat.at[1 - dx, 1 - ds], halo_send.at[i], halo_recv.at[i],
                          head=away(x, dx, nx), seq=away(s, ds, nseq))
        goes, comes = s >= 0, s >= 0
        if ds:
            goes = goes & (s + ds >= 0) & (s + ds < nseq)
            comes = comes & (s - ds >= 0) & (s - ds < nseq)
        if dx:
            goes = goes & (x + 1 < nx)
            comes = comes & (x > 0)
        sends.append((copy, goes, comes))
    for copy, goes, comes in sends:
        @pl.when(goes)
        def _():
            copy().start()

    for i in range(3):
        all_but_one(i).wait_send()

    def drain(h, carry):
        for kv in range(2):
            for direction in (1, -1):
                @pl.when(h <= last_hop(kv, direction))
                def _():
                    hop(kv, direction, h, h - 1).wait_send()
        for direction in (1, -1):
            @pl.when(h <= w_last(direction))
            def _():
                w_hop(direction, h, h - 1).wait_send()
        return carry

    lax.fori_loop(1, half + 1, drain, 0)

    def drain_pair(zz, carry):
        for kv in range(2):
            share(kv, zz, c).wait_send()
        w_share(zz, c).wait_send()
        return carry

    lax.fori_loop(0, nz, drain_pair, 0)

    def drain_rs(t, carry):
        for f, direction in flows:
            rs(f, direction, t).wait_send()
        return carry

    lax.fori_loop(1, nx, drain_rs, 0)
    for copy, goes, comes in sends:
        @pl.when(comes)
        def _():
            copy().wait_recv()
    lat_ref[...] = lat[...]
    for copy, goes, comes in sends:
        @pl.when(goes)
        def _():
            copy().wait_send()
    out.wait()


def transformer_part(queries, attn_keys, attn_values, residual, out_weight, out_gate,
                     head_shift, head_scale, head_weight, head_bias):
    nx, nz = lax.axis_size("head"), lax.axis_size("seq") // 2
    frames, height, breadth, features = queries.shape
    model = residual.shape[3]
    rows, width = frames * height * breadth, features // nx
    heads = width // HEAD_DIM
    count = rows * nx
    share_cols = out_weight.shape[1]
    cells = head_weight.shape[1]
    there = pl.BlockSpec(memory_space=pltpu.HBM)
    vmem = pl.BlockSpec(memory_space=pltpu.VMEM)
    dma = pltpu.SemaphoreType.DMA
    bf, f32 = jnp.bfloat16, jnp.float32
    block = model // (2 * SUBS)
    return pl.pallas_call(
        functools.partial(block_kernel, nx, nz),
        out_shape=(jax.ShapeDtypeStruct((rows, model), bf), jax.ShapeDtypeStruct((2, 3, rows, 2 * cells), bf)),
        in_specs=[there] * 10,
        out_specs=(there, vmem),
        scratch_shapes=[
            pltpu.VMEM((count, width), bf),
            pltpu.VMEM((2, nz, count, width), bf),
            pltpu.VMEM((2, nz, count, width), bf),
            pltpu.VMEM((nz, 2, share_cols, width), bf),
            pltpu.VMEM((heads, HEAD_DIM, count), bf),
            pltpu.VMEM((heads, HEAD_DIM, count), f32),
            pltpu.VMEM((heads, 2, 1, count), f32),
            pltpu.VMEM((count, model), f32),
            pltpu.VMEM((2 * SUBS, nx, rows, block), bf),
            pltpu.VMEM((2 * SUBS, nx, rows, block), bf),
            pltpu.VMEM((count, width), bf),
            pltpu.VMEM((rows, model), bf),
            pltpu.VMEM((2, 3, rows, 2 * cells), bf),
            pltpu.VMEM((rows, model), bf),
            pltpu.VMEM((1, model), f32),
            pltpu.VMEM((1, model), f32),
            pltpu.VMEM((1, model), f32),
            pltpu.VMEM((model, cells), bf),
            pltpu.VMEM((1, cells), f32),
            dma((10,)), dma((3,)), dma((3,)),
            dma((4, nz // 2 + 1)), dma((4, nz // 2 + 1)),
            dma((2, nz)), dma((2, nz)),
            dma((2, nz // 2 + 1)), dma((2, nz // 2 + 1)),
            dma((nz,)), dma((nz,)),
            dma((2 * SUBS, nx)), dma((2 * SUBS, nx)),
            dma((5,)), dma((5,)), dma((1,)),
        ],
        compiler_params=pltpu.CompilerParams(
            collective_id=0, has_side_effects=True, vmem_limit_bytes=56 * 2**20),
        cost_estimate=pl.CostEstimate(flops=4 * count * count * 2 * nz * width, bytes_accessed=2**21, transcendentals=0),
        name="block_ring",
    )(queries.reshape(rows, features), attn_keys.reshape(rows, features), attn_values.reshape(rows, features),
      out_weight.T, residual.reshape(rows, model), out_gate.reshape(1, model), head_shift.reshape(1, model),
      head_scale.reshape(1, model), head_weight, head_bias.reshape(1, cells))


def on_device(queries, attn_keys, attn_values, residual, out_weight, out_gate, head_shift, head_scale,
              head_weight, head_bias, conv_weight, conv_bias, norm_gain):
    frames, height, breadth = queries.shape[:3]
    channels = head_weight.shape[1] // 4
    hidden, lat = transformer_part(queries, attn_keys, attn_values, residual, out_weight, out_gate,
                                   head_shift, head_scale, head_weight, head_bias)
    cells = lat[..., : 4 * channels].reshape(2, 3, frames, breadth, 2, 2, channels)
    video = cells.transpose(0, 2, 1, 4, 3, 5, 6).reshape(2 * frames, 6, 2 * breadth, channels)[:, 1:5]
    padded = jnp.pad(video, ((0, 0), (0, 0), (1, 1), (0, 0)))
    features = convolve(padded, frames, conv_weight, conv_bias, norm_gain)
    return hidden.reshape(residual.shape), features


def solution(mesh):
    return jax.shard_map(
        on_device,
        mesh=mesh,
        in_specs=(
            P(("clip", "head"), "seq", None, None),
            P(("clip", "head"), "seq", None, None),
            P(("clip", "head"), "seq", None, None),
            P(("clip", "head"), "seq", None, None),
            P("head", "seq"),
            P(),
            P(),
            P(),
            P(),
            P(),
            P(),
            P(),
            P(),
        ),
        out_specs=(P(("clip", "head"), "seq", None, None), P(("clip", "head"), "seq", None, None)),
        check_vma=False,
    )
```

```python
import functools

import jax
import jax.numpy as jnp
from jax import lax
from jax.experimental import pallas as pl
from jax.experimental.pallas import tpu as pltpu
from jax.sharding import PartitionSpec as P

HEAD_DIM = 128
MESH = pl.DeviceIdType.MESH
SUBS = 2


def convolve(padded, frames, conv_weight, conv_bias, norm_gain):
    height = padded.shape[1] - 2
    breadth = padded.shape[2] - 2
    stacked = jnp.concatenate(
        [
            padded[
                time_off : time_off + frames,
                row_off : row_off + height,
                col_off : col_off + breadth,
            ]
            for time_off in range(3)
            for row_off in range(3)
            for col_off in range(3)
        ],
        -1,
    )
    kernel = conv_weight.reshape(-1, conv_weight.shape[-1])
    linear = (
        jnp.dot(stacked.reshape(-1, stacked.shape[-1]), kernel, preferred_element_type=jnp.float32)
        + conv_bias
    )
    normed = linear * lax.rsqrt(jnp.mean(linear * linear, -1, keepdims=True) + 1e-06) * norm_gain
    return jax.nn.silu(normed).astype(jnp.bfloat16).reshape(frames, height, breadth, -1)


def block_kernel(nx, nz, q_in, k_in, v_in, w_in, res_in, gate_in, shift_in, scale_in, hw_in, hb_in,
                 hidden_ref, lat_ref,
                 qa, ka, va, qp, kp, vp, wbuf, qt, acc, stat, part, sums_out, sums_in, tokens, plane_out, owned, lat,
                 res, gate, shift, gain, hw, hb,
                 local_sem, a2a_send, a2a_recv, ring_send, ring_recv, pair_send, pair_recv,
                 pring_send, pring_recv, ppair_send, ppair_recv, back_send, back_recv,
                 w_send, w_recv, wpair_send, wpair_recv, rs_send, rs_recv, halo_send, halo_recv, out_sem):
    x = lax.axis_index("head")
    s = lax.axis_index("seq")
    z, c = s // 2, lax.rem(s, 2)
    nseq = 2 * nz
    rows, width = k_in.shape[0], tokens.shape[1]
    scale = HEAD_DIM ** (-0.5)
    halfz, halfx = nz // 2, nx // 2
    features = part.shape[1]
    queries = qt.shape[2]

    def away(value, by, size):
        return lax.rem(value + by + 2 * size, size)

    def seq_of(zz, cc):
        return away(zz, 0, nz) * 2 + cc

    def remote(src, dst, send, recv, **where):
        return pltpu.make_async_remote_copy(
            src_ref=src, dst_ref=dst, send_sem=send, recv_sem=recv, device_id=where, device_id_type=MESH)

    def span(i, size):
        return pl.ds(pl.multiple_of(i * size, size), size)

    def column_head(xx):
        return span(xx * (width // HEAD_DIM), HEAD_DIM)

    def plane_head(zz):
        return span((zz // 2) * (width // HEAD_DIM) + 1 + lax.rem(zz, 2), HEAD_DIM)

    ins = (k_in, v_in, q_in)
    col_dst = (ka.at[c, z], va.at[c, z], qa)
    plane_dst = (kp.at[c, x], vp.at[c, x], qp)
    loads = [pltpu.make_async_copy(ins[i].at[:, column_head(x)], col_dst[i].at[span(x, rows), :], local_sem.at[i])
             for i in range(3)]
    loads += [pltpu.make_async_copy(ins[i].at[:, plane_head(z)], plane_dst[i].at[span(z, rows), :], local_sem.at[3 + i])
              for i in range(3)]
    w_load = pltpu.make_async_copy(w_in, wbuf.at[z, c], local_sem.at[6])
    late = ((res_in, res), (gate_in, gate), (shift_in, shift), (scale_in, gain), (hw_in, hw), (hb_in, hb))
    late = [pltpu.make_async_copy(a, b, local_sem.at[7 + i]) for i, (a, b) in enumerate(late)]
    for load in loads + [w_load] + late:
        load.start()
    lat[...] = jnp.zeros_like(lat)

    alone = (z // 2 == x).astype(jnp.int32)
    barrier = pltpu.get_barrier_semaphore()

    def greet(**where):
        pl.semaphore_signal(barrier, inc=1, device_id=where, device_id_type=MESH)

    for d in range(1, nx):
        greet(head=away(x, d, nx))
    for d in range(1, nz):
        greet(seq=seq_of(z + d, c))
    for other in (seq_of(z, 1 - c), away(s, 2 * c - 1, nseq)):
        greet(seq=other)
    for dx in (1, -1):
        for ds in (1, -1):
            greet(head=away(x, dx, nx), seq=away(s, ds, nseq))
    for xx in range(nx):
        for half in range(2):
            @pl.when(jnp.logical_or(x != xx, z != 2 * x + half))
            def _():
                greet(head=xx, seq=seq_of(2 * x + half, c))
    pl.semaphore_wait(barrier, nx - 1 + nz - 1 + 2 + 4 + 2 * nx - alone)

    def far_first(size):
        return sorted(range(1, size), key=lambda d: -min(d, size - d))

    def exchange(i):
        for d in far_first(nz):
            to = away(z, d, nz)
            remote(ins[i].at[:, plane_head(to)], plane_dst[i].at[span(z, rows), :],
                   a2a_send.at[3 + i], a2a_recv.at[3 + i], seq=seq_of(to, c)).start()
        for d in far_first(nx):
            to = away(x, d, nx)
            remote(ins[i].at[:, column_head(to)], col_dst[i].at[span(x, rows), :],
                   a2a_send.at[i], a2a_recv.at[i], head=to).start()

    for i in range(3):
        exchange(i)

    def from_column(i):
        piece = col_dst[i].at[pl.ds(0, rows * (nx - 1)), :]
        return remote(piece, piece, a2a_send.at[i], a2a_recv.at[i], head=away(x, 1, nx))

    def from_plane(i):
        piece = plane_dst[i].at[pl.ds(0, rows * (nz - 1)), :]
        return remote(piece, piece, a2a_send.at[3 + i], a2a_recv.at[3 + i], seq=seq_of(z + 1, c))

    col_kv, plane_kv = (ka, va), (kp, vp)

    def flow_of(kv, direction):
        return 2 * kv + (1 if direction > 0 else 0)

    def hop(kv, direction, step, back):
        slot, flow = col_kv[kv].at[c, away(z, -direction * back, nz)], flow_of(kv, direction)
        return remote(slot, slot, ring_send.at[flow, step], ring_recv.at[flow, step], seq=seq_of(z + direction, c))

    def share(kv, zz, cc):
        slot = col_kv[kv].at[cc, zz]
        return remote(slot, slot, pair_send.at[kv, zz], pair_recv.at[kv, zz], seq=seq_of(z, 1 - c))

    def phop(kv, direction, step, back):
        slot, flow = plane_kv[kv].at[c, away(x, -direction * back, nx)], flow_of(kv, direction)
        return remote(slot, slot, pring_send.at[flow, step], pring_recv.at[flow, step], head=away(x, direction, nx))

    def pshare(kv, xx, cc):
        slot = plane_kv[kv].at[cc, xx]
        return remote(slot, slot, ppair_send.at[kv, xx], ppair_recv.at[kv, xx], seq=seq_of(z, 1 - c))

    def w_hop(direction, step, back):
        slot, flow = wbuf.at[away(z, -direction * back, nz), c], 1 if direction > 0 else 0
        return remote(slot, slot, w_send.at[flow, step], w_recv.at[flow, step], seq=seq_of(z + direction, c))

    def w_share(zz, cc):
        slot = wbuf.at[zz, cc]
        return remote(slot, slot, wpair_send.at[zz], wpair_recv.at[zz], seq=seq_of(z, 1 - c))

    def last_hop(kv, direction, half):
        return half if (kv == 0) == (direction > 0) else half - 1

    def w_last(direction):
        return halfz if direction > 0 else halfz - 1

    def w_step(h):
        for direction in (1, -1):
            @pl.when(h <= w_last(direction))
            def _():
                w_hop(direction, h, h).wait_recv()

                @pl.when(h < w_last(direction))
                def _():
                    w_hop(direction, h + 1, h).start()

                w_share(away(z, -direction * h, nz), c).start()

    def col_step(h):
        for kv in range(2):
            for direction in (1, -1):
                @pl.when(h <= last_hop(kv, direction, halfz))
                def _():
                    hop(kv, direction, h, h).wait_recv()

                    @pl.when(h < last_hop(kv, direction, halfz))
                    def _():
                        hop(kv, direction, h + 1, h).start()

                    share(kv, away(z, -direction * h, nz), c).start()

    def plane_step(h):
        for kv in range(2):
            for direction in (1, -1):
                @pl.when(h <= last_hop(kv, direction, halfx))
                def _():
                    phop(kv, direction, h, h).wait_recv()

                    @pl.when(h < last_hop(kv, direction, halfx))
                    def _():
                        phop(kv, direction, h + 1, h).start()

                    pshare(kv, away(x, -direction * h, nx), c).start()

    def fold(j, keys, values):
        scores = [lax.dot_general(key[...], qt[j], (((1,), (0,)), ((), ())), preferred_element_type=jnp.float32)
                  for key in keys]
        before = stat[j, 0]
        peak = before
        for part_scores in scores:
            peak = jnp.maximum(peak, jnp.max(part_scores, 0, keepdims=True))
        factor = jnp.exp((before - peak) * scale)
        total, product = stat[j, 1] * factor, acc[j] * factor
        for part_scores, value in zip(scores, values):
            weights = jnp.exp((part_scores - peak) * scale)
            total = total + jnp.sum(weights, 0, keepdims=True)
            product = product + lax.dot_general(value[...], weights.astype(jnp.bfloat16), (((0,), (0,)), ((), ())),
                                                preferred_element_type=jnp.float32)
        stat[j, 0], stat[j, 1], acc[j] = peak, total, product

    def col_attend(zs):
        for zz in zs:
            for kv in range(2):
                share(kv, zz, 1 - c).wait_recv()
        fold(0, [ka.at[lane, zz] for zz in zs for lane in range(2)], [va.at[lane, zz] for zz in zs for lane in range(2)])

    def col_attend_at(h):
        col_attend([away(z, -h, nz), away(z, h, nz)])

    def plane_attend(xx):
        for kv in range(2):
            pshare(kv, xx, 1 - c).wait_recv()

        def part_of_queries(j, carry):
            fold(j, [kp.at[lane, xx] for lane in range(2)], [vp.at[lane, xx] for lane in range(2)])
            return carry

        lax.fori_loop(1, qt.shape[0], part_of_queries, 0)

    def plane_attend_at(h):
        def side(i, carry):
            plane_attend(away(x, (2 * i - 1) * h, nx))
            return carry

        lax.fori_loop(0, 2, side, 0)

    w_load.wait()
    for direction in (1, -1):
        w_hop(direction, 1, 0).start()
    w_share(z, c).start()
    for kv in range(2):
        loads[3 + kv].wait()
        from_plane(kv).wait_recv()
        for direction in (1, -1):
            if last_hop(kv, direction, halfx) >= 1:
                phop(kv, direction, 1, 0).start()
        pshare(kv, x, c).start()
    for kv in range(2):
        loads[kv].wait()
        from_column(kv).wait_recv()
        for direction in (1, -1):
            hop(kv, direction, 1, 0).start()
        share(kv, z, c).start()
    for i, dst in ((2, qa), (5, qp)):
        loads[i].wait()
    from_column(2).wait_recv()
    from_plane(2).wait_recv()
    w_step(1)

    acc[...] = jnp.zeros_like(acc)
    stat[:, 0] = jnp.full(stat[:, 0].shape, -1e30, jnp.float32)
    stat[:, 1] = jnp.zeros_like(stat[:, 1])
    qt[0] = qa[...].astype(jnp.float32).T.astype(jnp.bfloat16)
    for j in range(1, qt.shape[0]):
        qt[j] = qp[(j - 1) * queries:j * queries, :].astype(jnp.float32).T.astype(jnp.bfloat16)
    col_attend([z])
    plane_attend(x)
    w_step(2)

    def step(i, carry):
        col_step(2 * i - 1)

        @pl.when(i > 1)
        def _():
            col_attend_at(2 * i - 2)

        plane_step(i)
        col_step(2 * i)
        col_attend_at(2 * i - 1)
        w_step(i + 2)
        plane_attend_at(i)
        return carry

    lax.fori_loop(1, halfx, step, 0)
    col_step(halfz - 1)
    if halfz > 2:
        col_attend_at(halfz - 2)
    plane_step(halfx)
    plane_attend(away(x, halfx, nx))

    for j in range(1, qt.shape[0]):
        plane_out[(j - 1) * queries:j * queries, :] = (acc[j] / stat[j, 1]).T.astype(jnp.bfloat16)
    group, which = z // 2, lax.rem(z, 2)

    def back(zz, xx, part_of):
        return remote(plane_out.at[span(zz, rows), :], tokens.at[span(xx, rows), span(1 + part_of, HEAD_DIM)],
                      back_send.at[zz], back_recv.at[2 * xx + part_of], head=group, seq=seq_of(zz, c))

    for d in far_first(nz) + [0]:
        zz = away(z, d, nz)
        if d:
            back(zz, x, which).start()
        else:
            @pl.when(alone == 0)
            def _():
                back(zz, x, which).start()

            @pl.when(alone == 1)
            def _():
                tokens[span(x, rows), span(1 + which, HEAD_DIM)] = plane_out[span(zz, rows), :]

    col_step(halfz)
    col_attend_at(halfz - 1)
    col_attend([away(z, halfz, nz)])
    tokens[:, 0:HEAD_DIM] = (acc[0] / stat[0, 1]).T.astype(jnp.bfloat16)
    for h in range(halfx + 2, halfz + 1):
        w_step(h)

    def w_land(zz, carry):
        w_share(zz, 1 - c).wait_recv()
        return carry

    lax.fori_loop(0, nz, w_land, 0)
    for xx in range(nx):
        for part_of in range(2):
            @pl.when(jnp.logical_or(alone == 0, jnp.logical_or(x != xx, which != part_of)))
            def _():
                back(z, xx, part_of).wait_recv()

    w_rows = w_in.shape[0]
    tile = 4 * w_rows

    def project(i, carry):
        columns = wbuf[pl.ds(2 * i, 2)].reshape(tile, width)
        part[:, span(i, tile)] = lax.dot_general(
            tokens[...], columns, (((1,), (1,)), ((), ())), preferred_element_type=jnp.float32)
        return carry

    lax.fori_loop(0, nz // 2, project, 0)
    block = features // (2 * SUBS)

    def term(flow, direction, t):
        owner = away(x, -direction * t, nx)
        return part[span(owner, rows), flow * block:(flow + 1) * block]

    def rs(flow, direction, t):
        return remote(sums_out.at[flow, t], sums_in.at[flow, t], rs_send.at[flow, t], rs_recv.at[flow, t],
                      head=away(x, direction, nx))

    flows = [(f, 1 if f % 2 else -1) for f in range(2 * SUBS)]
    for f, direction in flows:
        sums_out[f, 1] = term(f, direction, 1).astype(jnp.bfloat16)
    for f, direction in flows:
        rs(f, direction, 1).start()

    def rs_step(t, carry):
        for f, direction in flows:
            rs(f, direction, t - 1).wait_recv()
            sums_out[f, t] = (sums_in[f, t - 1].astype(jnp.float32) + term(f, direction, t)).astype(jnp.bfloat16)
            rs(f, direction, t).start()
        return carry

    lax.fori_loop(2, nx, rs_step, 0)
    for load in late:
        load.wait()
    for f, direction in flows:
        rs(f, direction, nx - 1).wait_recv()
        cols = slice(f * block, (f + 1) * block)
        total = sums_in[f, nx - 1].astype(jnp.float32) + term(f, direction, nx)
        owned[:, cols] = (res[:, cols].astype(jnp.float32) + gate[:, cols] * total).astype(jnp.bfloat16)

    out = pltpu.make_async_copy(owned, hidden_ref, out_sem.at[0])
    out.start()
    values = owned[...].astype(jnp.float32)
    center = values - jnp.mean(values, -1, keepdims=True)
    spread = jnp.mean(center * center, -1, keepdims=True)
    normed = (center * lax.rsqrt(spread + 1e-06) * (1.0 + gain[...]) + shift[...]).astype(jnp.bfloat16)
    latent = jnp.dot(normed, hw[...], preferred_element_type=jnp.float32) + hb[...]
    cells = latent.shape[1]
    lat[1, 1, :, 0:cells] = latent.astype(jnp.bfloat16)

    sends = []
    for i, (dx, ds) in enumerate(((0, 1), (0, -1), (1, 0), (1, 1), (1, -1))):
        def copy(i=i, dx=dx, ds=ds):
            return remote(lat.at[1, 1], lat.at[1 - dx, 1 - ds], halo_send.at[i], halo_recv.at[i],
                          head=away(x, dx, nx), seq=away(s, ds, nseq))
        goes, comes = s >= 0, s >= 0
        if ds:
            goes = goes & (s + ds >= 0) & (s + ds < nseq)
            comes = comes & (s - ds >= 0) & (s - ds < nseq)
        if dx:
            goes = goes & (x + 1 < nx)
            comes = comes & (x > 0)
        sends.append((copy, goes, comes))
    for copy, goes, comes in sends:
        @pl.when(goes)
        def _():
            copy().start()

    for i in range(3):
        from_column(i).wait_send()
        from_plane(i).wait_send()

    def drain(h, carry):
        for kv in range(2):
            for direction in (1, -1):
                @pl.when(h <= last_hop(kv, direction, halfz))
                def _():
                    hop(kv, direction, h, h - 1).wait_send()

                @pl.when(h <= last_hop(kv, direction, halfx))
                def _():
                    phop(kv, direction, h, h - 1).wait_send()
        for direction in (1, -1):
            @pl.when(h <= w_last(direction))
            def _():
                w_hop(direction, h, h - 1).wait_send()
        return carry

    lax.fori_loop(1, halfz + 1, drain, 0)

    def drain_pair(zz, carry):
        for kv in range(2):
            share(kv, zz, c).wait_send()

            @pl.when(zz < nx)
            def _():
                pshare(kv, zz, c).wait_send()
        w_share(zz, c).wait_send()

        @pl.when(jnp.logical_or(alone == 0, zz != z))
        def _():
            back(zz, x, which).wait_send()
        return carry

    lax.fori_loop(0, nz, drain_pair, 0)

    def drain_rs(t, carry):
        for f, direction in flows:
            rs(f, direction, t).wait_send()
        return carry

    lax.fori_loop(1, nx, drain_rs, 0)
    for copy, goes, comes in sends:
        @pl.when(comes)
        def _():
            copy().wait_recv()
    lat_ref[...] = lat[...]
    for copy, goes, comes in sends:
        @pl.when(goes)
        def _():
            copy().wait_send()
    out.wait()


def transformer_part(queries, attn_keys, attn_values, residual, out_weight, out_gate,
                     head_shift, head_scale, head_weight, head_bias):
    nx, nz = lax.axis_size("head"), lax.axis_size("seq") // 2
    frames, height, breadth, features = queries.shape
    model = residual.shape[3]
    rows, width = frames * height * breadth, features // nx
    heads = width // HEAD_DIM
    count = rows * nx
    planes = rows * nz
    share_cols = out_weight.shape[1]
    if nz != 2 * nx or heads != 3:
        raise ValueError("unsupported mesh")
    cells = head_weight.shape[1]
    there = pl.BlockSpec(memory_space=pltpu.HBM)
    vmem = pl.BlockSpec(memory_space=pltpu.VMEM)
    dma = pltpu.SemaphoreType.DMA
    bf, f32 = jnp.bfloat16, jnp.float32
    block = model // (2 * SUBS)
    return pl.pallas_call(
        functools.partial(block_kernel, nx, nz),
        out_shape=(jax.ShapeDtypeStruct((rows, model), bf), jax.ShapeDtypeStruct((2, 3, rows, 2 * cells), bf)),
        in_specs=[there] * 10,
        out_specs=(there, vmem),
        scratch_shapes=[
            pltpu.VMEM((count, HEAD_DIM), bf),
            pltpu.VMEM((2, nz, count, HEAD_DIM), bf),
            pltpu.VMEM((2, nz, count, HEAD_DIM), bf),
            pltpu.VMEM((planes, HEAD_DIM), bf),
            pltpu.VMEM((2, nx, planes, HEAD_DIM), bf),
            pltpu.VMEM((2, nx, planes, HEAD_DIM), bf),
            pltpu.VMEM((nz, 2, share_cols, width), bf),
            pltpu.VMEM((heads, HEAD_DIM, count), bf),
            pltpu.VMEM((heads, HEAD_DIM, count), f32),
            pltpu.VMEM((heads, 2, 1, count), f32),
            pltpu.VMEM((count, model), f32),
            pltpu.VMEM((2 * SUBS, nx, rows, block), bf),
            pltpu.VMEM((2 * SUBS, nx, rows, block), bf),
            pltpu.VMEM((count, width), bf),
            pltpu.VMEM((planes, HEAD_DIM), bf),
            pltpu.VMEM((rows, model), bf),
            pltpu.VMEM((2, 3, rows, 2 * cells), bf),
            pltpu.VMEM((rows, model), bf),
            pltpu.VMEM((1, model), f32),
            pltpu.VMEM((1, model), f32),
            pltpu.VMEM((1, model), f32),
            pltpu.VMEM((model, cells), bf),
            pltpu.VMEM((1, cells), f32),
            dma((13,)), dma((6,)), dma((6,)),
            dma((4, nz // 2 + 1)), dma((4, nz // 2 + 1)),
            dma((2, nz)), dma((2, nz)),
            dma((4, nx // 2 + 1)), dma((4, nx // 2 + 1)),
            dma((2, nx)), dma((2, nx)),
            dma((nz,)), dma((2 * nx,)),
            dma((2, nz // 2 + 1)), dma((2, nz // 2 + 1)),
            dma((nz,)), dma((nz,)),
            dma((2 * SUBS, nx)), dma((2 * SUBS, nx)),
            dma((5,)), dma((5,)), dma((1,)),
        ],
        compiler_params=pltpu.CompilerParams(
            collective_id=0, has_side_effects=True, vmem_limit_bytes=56 * 2**20),
        cost_estimate=pl.CostEstimate(flops=4 * count * count * 2 * nz * width, bytes_accessed=2**21, transcendentals=0),
        name="block_ring",
    )(queries.reshape(rows, features), attn_keys.reshape(rows, features), attn_values.reshape(rows, features),
      out_weight.T, residual.reshape(rows, model), out_gate.reshape(1, model), head_shift.reshape(1, model),
      head_scale.reshape(1, model), head_weight, head_bias.reshape(1, cells))


def on_device(queries, attn_keys, attn_values, residual, out_weight, out_gate, head_shift, head_scale,
              head_weight, head_bias, conv_weight, conv_bias, norm_gain):
    frames, height, breadth = queries.shape[:3]
    channels = head_weight.shape[1] // 4
    hidden, lat = transformer_part(queries, attn_keys, attn_values, residual, out_weight, out_gate,
                                   head_shift, head_scale, head_weight, head_bias)
    cells = lat[..., : 4 * channels].reshape(2, 3, frames, breadth, 2, 2, channels)
    video = cells.transpose(0, 2, 1, 4, 3, 5, 6).reshape(2 * frames, 6, 2 * breadth, channels)[:, 1:5]
    padded = jnp.pad(video, ((0, 0), (0, 0), (1, 1), (0, 0)))
    features = convolve(padded, frames, conv_weight, conv_bias, norm_gain)
    return hidden.reshape(residual.shape), features


def solution(mesh):
    return jax.shard_map(
        on_device,
        mesh=mesh,
        in_specs=(
            P(("clip", "head"), "seq", None, None),
            P(("clip", "head"), "seq", None, None),
            P(("clip", "head"), "seq", None, None),
            P(("clip", "head"), "seq", None, None),
            P("head", "seq"),
            P(),
            P(),
            P(),
            P(),
            P(),
            P(),
            P(),
            P(),
        ),
        out_specs=(P(("clip", "head"), "seq", None, None), P(("clip", "head"), "seq", None, None)),
        check_vma=False,
    )
```

```python
import functools

import jax
import jax.numpy as jnp
from jax import lax
from jax.experimental import pallas as pl
from jax.experimental.pallas import tpu as pltpu
from jax.sharding import PartitionSpec as P

HEAD_DIM = 128
MESH = pl.DeviceIdType.MESH


def convolve(padded, frames, conv_weight, conv_bias, norm_gain):
    height = padded.shape[1] - 2
    breadth = padded.shape[2] - 2
    stacked = jnp.concatenate(
        [
            padded[
                time_off : time_off + frames,
                row_off : row_off + height,
                col_off : col_off + breadth,
            ]
            for time_off in range(3)
            for row_off in range(3)
            for col_off in range(3)
        ],
        -1,
    )
    kernel = conv_weight.reshape(-1, conv_weight.shape[-1])
    linear = (
        jnp.dot(stacked.reshape(-1, stacked.shape[-1]), kernel, preferred_element_type=jnp.float32)
        + conv_bias
    )
    normed = linear * lax.rsqrt(jnp.mean(linear * linear, -1, keepdims=True) + 1e-06) * norm_gain
    return jax.nn.silu(normed).astype(jnp.bfloat16).reshape(frames, height, breadth, -1)


def block_kernel(nx, nz, q_in, k_in, v_in, w_in, res_in, gate_in, shift_in, scale_in, hw_in, hb_in,
                 hidden_ref, lat_ref,
                 qa, ka, va, qp, kp, vp, wbuf, qt, acc, stat, part, sums_out, sums_in, tokens, plane_out, owned, lat,
                 res, gate, shift, gain, hw, hb,
                 local_sem, a2a_send, a2a_recv, ring_send, ring_recv, pair_send, pair_recv,
                 pring_send, pring_recv, ppair_send, ppair_recv, back_send, back_recv,
                 w_send, w_recv, wpair_send, wpair_recv, rs_send, rs_recv, halo_send, halo_recv, out_sem):
    x = lax.axis_index("head")
    s = lax.axis_index("seq")
    z, c = s // 2, lax.rem(s, 2)
    nseq = 2 * nz
    rows, width = k_in.shape[0], tokens.shape[1]
    scale = HEAD_DIM ** (-0.5) * 1.4426950408889634
    halfz, halfx = nz // 2, nx // 2
    queries = qt.shape[2]

    def away(value, by, size):
        return lax.rem(value + by + 2 * size, size)

    def seq_of(zz, cc):
        return away(zz, 0, nz) * 2 + cc

    def remote(src, dst, send, recv, **where):
        return pltpu.make_async_remote_copy(
            src_ref=src, dst_ref=dst, send_sem=send, recv_sem=recv, device_id=where, device_id_type=MESH)

    def span(i, size):
        return pl.ds(pl.multiple_of(i * size, size), size)

    def column_head(xx):
        return span(xx * (width // HEAD_DIM), HEAD_DIM)

    def plane_head(zz):
        return span((zz // 2) * (width // HEAD_DIM) + 1 + lax.rem(zz, 2), HEAD_DIM)

    ins = (k_in, v_in, q_in)
    col_dst = (ka.at[c, z], va.at[c, z], qa)
    plane_dst = (kp.at[c, x], vp.at[c, x], qp)
    loads = [pltpu.make_async_copy(ins[i].at[:, column_head(x)], col_dst[i].at[span(x, rows), :], local_sem.at[i])
             for i in range(3)]
    loads += [pltpu.make_async_copy(ins[i].at[:, plane_head(z)], plane_dst[i].at[span(z, rows), :], local_sem.at[3 + i])
              for i in range(3)]
    w_load = pltpu.make_async_copy(w_in, wbuf.at[z, c], local_sem.at[6])
    late = ((res_in, res), (gate_in, gate), (shift_in, shift), (scale_in, gain), (hw_in, hw), (hb_in, hb))
    late = [pltpu.make_async_copy(a, b, local_sem.at[7 + i]) for i, (a, b) in enumerate(late)]
    for load in loads + [w_load] + late:
        load.start()
    lat[...] = jnp.zeros_like(lat)

    alone = (z // 2 == x).astype(jnp.int32)
    barrier = pltpu.get_barrier_semaphore()

    def greet(**where):
        pl.semaphore_signal(barrier, inc=1, device_id=where, device_id_type=MESH)

    for d in range(1, nx):
        greet(head=away(x, d, nx))
    for d in range(1, nz):
        greet(seq=seq_of(z + d, c))
    for other in (seq_of(z, 1 - c), away(s, 2 * c - 1, nseq)):
        greet(seq=other)
    for dx in (1, -1):
        for ds in (1, -1):
            greet(head=away(x, dx, nx), seq=away(s, ds, nseq))
    for xx in range(nx):
        for half in range(2):
            @pl.when(jnp.logical_or(x != xx, z != 2 * x + half))
            def _():
                greet(head=xx, seq=seq_of(2 * x + half, c))
    pl.semaphore_wait(barrier, nx - 1 + nz - 1 + 2 + 4 + 2 * nx - alone)

    def far_first(size):
        return sorted(range(1, size), key=lambda d: -min(d, size - d))

    def exchange(i):
        for d in far_first(nz):
            to = away(z, d, nz)
            remote(ins[i].at[:, plane_head(to)], plane_dst[i].at[span(z, rows), :],
                   a2a_send.at[3 + i], a2a_recv.at[3 + i], seq=seq_of(to, c)).start()
        for d in far_first(nx):
            to = away(x, d, nx)
            remote(ins[i].at[:, column_head(to)], col_dst[i].at[span(x, rows), :],
                   a2a_send.at[i], a2a_recv.at[i], head=to).start()

    for i in range(3):
        exchange(i)

    def from_column(i):
        piece = col_dst[i].at[pl.ds(0, rows * (nx - 1)), :]
        return remote(piece, piece, a2a_send.at[i], a2a_recv.at[i], head=away(x, 1, nx))

    def from_plane(i):
        piece = plane_dst[i].at[pl.ds(0, rows * (nz - 1)), :]
        return remote(piece, piece, a2a_send.at[3 + i], a2a_recv.at[3 + i], seq=seq_of(z + 1, c))

    col_kv, plane_kv = (ka, va), (kp, vp)

    def flow_of(kv, direction):
        return 2 * kv + (1 if direction > 0 else 0)

    def hop(kv, direction, step, back):
        slot, flow = col_kv[kv].at[c, away(z, -direction * back, nz)], flow_of(kv, direction)
        return remote(slot, slot, ring_send.at[flow, step], ring_recv.at[flow, step], seq=seq_of(z + direction, c))

    def share(kv, zz, cc):
        slot = col_kv[kv].at[cc, zz]
        return remote(slot, slot, pair_send.at[kv, zz], pair_recv.at[kv, zz], seq=seq_of(z, 1 - c))

    def phop(kv, direction, step, back):
        slot, flow = plane_kv[kv].at[c, away(x, -direction * back, nx)], flow_of(kv, direction)
        return remote(slot, slot, pring_send.at[flow, step], pring_recv.at[flow, step], head=away(x, direction, nx))

    def pshare(kv, xx, cc):
        slot = plane_kv[kv].at[cc, xx]
        return remote(slot, slot, ppair_send.at[kv, xx], ppair_recv.at[kv, xx], seq=seq_of(z, 1 - c))

    def w_hop(direction, step, back):
        slot, flow = wbuf.at[away(z, -direction * back, nz), c], 1 if direction > 0 else 0
        return remote(slot, slot, w_send.at[flow, step], w_recv.at[flow, step], seq=seq_of(z + direction, c))

    def w_share(zz, cc):
        slot = wbuf.at[zz, cc]
        return remote(slot, slot, wpair_send.at[zz], wpair_recv.at[zz], seq=seq_of(z, 1 - c))

    def last_hop(kv, direction, half):
        return half if (kv == 0) == (direction > 0) else half - 1

    def w_last(direction):
        return halfz if direction > 0 else halfz - 1

    def w_step(h):
        for direction in (1, -1):
            @pl.when(h <= w_last(direction))
            def _():
                w_hop(direction, h, h).wait_recv()

                @pl.when(h < w_last(direction))
                def _():
                    w_hop(direction, h + 1, h).start()

                w_share(away(z, -direction * h, nz), c).start()

    def col_step(h):
        for kv in range(2):
            for direction in (1, -1):
                @pl.when(h <= last_hop(kv, direction, halfz))
                def _():
                    hop(kv, direction, h, h).wait_recv()

                    @pl.when(h < last_hop(kv, direction, halfz))
                    def _():
                        hop(kv, direction, h + 1, h).start()

                    share(kv, away(z, -direction * h, nz), c).start()

    def plane_step(h):
        for kv in range(2):
            for direction in (1, -1):
                @pl.when(h <= last_hop(kv, direction, halfx))
                def _():
                    phop(kv, direction, h, h).wait_recv()

                    @pl.when(h < last_hop(kv, direction, halfx))
                    def _():
                        phop(kv, direction, h + 1, h).start()

                    pshare(kv, away(x, -direction * h, nx), c).start()

    def fold(j, keys, values):
        scores = [lax.dot_general(key[...], qt[j], (((1,), (0,)), ((), ())), preferred_element_type=jnp.float32)
                  for key in keys]
        before = stat[j, 0]
        peak = before
        for part_scores in scores:
            peak = jnp.maximum(peak, jnp.max(part_scores, 0, keepdims=True))
        factor = jnp.exp2((before - peak) * scale)
        total, product = stat[j, 1] * factor, acc[j] * factor
        for part_scores, value in zip(scores, values):
            weights = jnp.exp2((part_scores - peak) * scale)
            total = total + jnp.sum(weights, 0, keepdims=True)
            product = product + lax.dot_general(value[...], weights.astype(jnp.bfloat16), (((0,), (0,)), ((), ())),
                                                preferred_element_type=jnp.float32)
        stat[j, 0], stat[j, 1], acc[j] = peak, total, product

    def col_attend(zs):
        for zz in zs:
            for kv in range(2):
                share(kv, zz, 1 - c).wait_recv()
        fold(0, [ka.at[lane, zz] for zz in zs for lane in range(2)], [va.at[lane, zz] for zz in zs for lane in range(2)])

    def col_attend_at(h):
        col_attend([away(z, -h, nz), away(z, h, nz)])

    def plane_attend(xx):
        for kv in range(2):
            pshare(kv, xx, 1 - c).wait_recv()

        for j in range(1, qt.shape[0]):
            fold(j, [kp.at[lane, xx] for lane in range(2)], [vp.at[lane, xx] for lane in range(2)])

    def plane_attend_at(h):
        def side(i, carry):
            plane_attend(away(x, (2 * i - 1) * h, nx))
            return carry

        lax.fori_loop(0, 2, side, 0)

    w_load.wait()
    for direction in (1, -1):
        w_hop(direction, 1, 0).start()
    w_share(z, c).start()
    for kv in range(2):
        loads[3 + kv].wait()
        from_plane(kv).wait_recv()
        for direction in (1, -1):
            if last_hop(kv, direction, halfx) >= 1:
                phop(kv, direction, 1, 0).start()
        pshare(kv, x, c).start()
    for kv in range(2):
        loads[kv].wait()
        from_column(kv).wait_recv()
        for direction in (1, -1):
            hop(kv, direction, 1, 0).start()
        share(kv, z, c).start()
    for i, dst in ((2, qa), (5, qp)):
        loads[i].wait()
    from_column(2).wait_recv()
    from_plane(2).wait_recv()
    w_step(1)

    acc[...] = jnp.zeros_like(acc)
    stat[:, 0] = jnp.full(stat[:, 0].shape, -1e30, jnp.float32)
    stat[:, 1] = jnp.zeros_like(stat[:, 1])
    qt[0] = qa[...].astype(jnp.float32).T.astype(jnp.bfloat16)
    for j in range(1, qt.shape[0]):
        qt[j] = qp[(j - 1) * queries:j * queries, :].astype(jnp.float32).T.astype(jnp.bfloat16)
    col_attend([z])
    plane_attend(x)
    w_step(2)
    w_at = [2]

    def w_reach(h):
        while w_at[0] < min(h, halfz):
            w_at[0] += 1
            w_step(w_at[0])

    def step(i, carry):
        col_step(2 * i - 1)

        @pl.when(i > 1)
        def _():
            col_attend_at(2 * i - 2)

        plane_step(i)
        col_step(2 * i)
        col_attend_at(2 * i - 1)
        plane_attend_at(i)
        return carry

    lax.fori_loop(1, halfx, step, 0)
    col_step(halfz - 1)
    w_reach(3)
    if halfz > 2:
        col_attend_at(halfz - 2)
    plane_step(halfx)
    plane_attend(away(x, halfx, nx))

    for j in range(1, qt.shape[0]):
        plane_out[(j - 1) * queries:j * queries, :] = (acc[j] / stat[j, 1]).T.astype(jnp.bfloat16)
    group, which = z // 2, lax.rem(z, 2)

    def back(zz, xx, part_of):
        return remote(plane_out.at[span(zz, rows), :], tokens.at[span(xx, rows), span(1 + part_of, HEAD_DIM)],
                      back_send.at[zz], back_recv.at[2 * xx + part_of], head=group, seq=seq_of(zz, c))

    for d in far_first(nz) + [0]:
        zz = away(z, d, nz)
        if d:
            back(zz, x, which).start()
        else:
            @pl.when(alone == 0)
            def _():
                back(zz, x, which).start()

            @pl.when(alone == 1)
            def _():
                tokens[span(x, rows), span(1 + which, HEAD_DIM)] = plane_out[span(zz, rows), :]

    w_reach(4)
    col_step(halfz)
    col_attend_at(halfz - 1)
    col_attend([away(z, halfz, nz)])
    tokens[:, 0:HEAD_DIM] = (acc[0] / stat[0, 1]).T.astype(jnp.bfloat16)
    w_reach(5)
    for xx in range(nx):
        for part_of in range(2):
            @pl.when(jnp.logical_or(alone == 0, jnp.logical_or(x != xx, which != part_of)))
            def _():
                back(z, xx, part_of).wait_recv()

    tile = 4 * w_in.shape[0]
    blocks = nz // 2
    order = sorted(range(1 - (blocks + 1) // 2, blocks // 2 + 1), key=lambda k: (abs(k), -k))
    flows = [(f, 1 if f % 2 == 0 else -1, away(z // 2, k, blocks)) for f, k in enumerate(order)]
    groups = [flows[g:g + 2] for g in range(0, blocks, 2)]
    reach = [max(min(2 * abs(order[f]) + 1, halfz) for f, _, _ in group) for group in groups]

    def project(block):
        for i in range(2):
            w_share(2 * block + i, 1 - c).wait_recv()
        columns = wbuf[pl.ds(2 * block, 2)].reshape(tile, width)
        part[:, span(block, tile)] = lax.dot_general(
            tokens[...], columns, (((1,), (1,)), ((), ())), preferred_element_type=jnp.float32)

    def term(direction, block, t):
        return part[span(away(x, -direction * t, nx), rows), span(block, tile)]

    def rs(f, direction, t):
        return remote(sums_out.at[f, t], sums_in.at[f, t], rs_send.at[f, t], rs_recv.at[f, t],
                      head=away(x, direction, nx))

    for turn in range(nx + len(groups) - 1):
        for g, group in enumerate(groups):
            t = turn - g + 1
            if t == 1:
                w_reach(reach[g])
                for f, direction, block in group:
                    project(block)
                for f, direction, block in group:
                    sums_out[f, 1] = term(direction, block, 1).astype(jnp.bfloat16)
                for f, direction, block in group:
                    rs(f, direction, 1).start()
            elif 1 < t < nx:
                for f, direction, block in group:
                    rs(f, direction, t - 1).wait_recv()
                    sums_out[f, t] = (sums_in[f, t - 1].astype(jnp.float32) + term(direction, block, t)).astype(jnp.bfloat16)
                    rs(f, direction, t).start()
            elif t == nx:
                if g == 0:
                    for load in late:
                        load.wait()
                for f, direction, block in group:
                    rs(f, direction, nx - 1).wait_recv()
                    total = sums_in[f, nx - 1].astype(jnp.float32) + term(direction, block, nx)
                    at = span(block, tile)
                    owned[:, at] = (res[:, at].astype(jnp.float32) + gate[:, at] * total).astype(jnp.bfloat16)
        w_reach(6 + turn)

    out = pltpu.make_async_copy(owned, hidden_ref, out_sem.at[0])
    out.start()
    values = owned[...].astype(jnp.float32)
    center = values - jnp.mean(values, -1, keepdims=True)
    spread = jnp.mean(center * center, -1, keepdims=True)
    normed = (center * lax.rsqrt(spread + 1e-06) * (1.0 + gain[...]) + shift[...]).astype(jnp.bfloat16)
    latent = lax.dot_general(normed, hw[...], (((1,), (1,)), ((), ())), preferred_element_type=jnp.float32) + hb[...]
    cells = latent.shape[1]
    lat[1, 1, :, 0:cells] = latent.astype(jnp.bfloat16)

    sends = []
    for i, (dx, ds) in enumerate(((0, 1), (0, -1), (1, 0), (1, 1), (1, -1))):
        def copy(i=i, dx=dx, ds=ds):
            return remote(lat.at[1, 1], lat.at[1 - dx, 1 - ds], halo_send.at[i], halo_recv.at[i],
                          head=away(x, dx, nx), seq=away(s, ds, nseq))
        goes, comes = s >= 0, s >= 0
        if ds:
            goes = goes & (s + ds >= 0) & (s + ds < nseq)
            comes = comes & (s - ds >= 0) & (s - ds < nseq)
        if dx:
            goes = goes & (x + 1 < nx)
            comes = comes & (x > 0)
        sends.append((copy, goes, comes))
    for copy, goes, comes in sends:
        @pl.when(goes)
        def _():
            copy().start()

    for i in range(3):
        from_column(i).wait_send()
        from_plane(i).wait_send()

    def drain(h, carry):
        for kv in range(2):
            for direction in (1, -1):
                @pl.when(h <= last_hop(kv, direction, halfz))
                def _():
                    hop(kv, direction, h, h - 1).wait_send()

                @pl.when(h <= last_hop(kv, direction, halfx))
                def _():
                    phop(kv, direction, h, h - 1).wait_send()
        for direction in (1, -1):
            @pl.when(h <= w_last(direction))
            def _():
                w_hop(direction, h, h - 1).wait_send()
        return carry

    lax.fori_loop(1, halfz + 1, drain, 0)

    def drain_pair(zz, carry):
        for kv in range(2):
            share(kv, zz, c).wait_send()

            @pl.when(zz < nx)
            def _():
                pshare(kv, zz, c).wait_send()
        w_share(zz, c).wait_send()

        @pl.when(jnp.logical_or(alone == 0, zz != z))
        def _():
            back(zz, x, which).wait_send()
        return carry

    lax.fori_loop(0, nz, drain_pair, 0)

    def drain_rs(t, carry):
        for f, direction, block in flows:
            rs(f, direction, t).wait_send()
        return carry

    lax.fori_loop(1, nx, drain_rs, 0)
    for copy, goes, comes in sends:
        @pl.when(comes)
        def _():
            copy().wait_recv()
    lat_ref[...] = lat[...]
    for copy, goes, comes in sends:
        @pl.when(goes)
        def _():
            copy().wait_send()
    out.wait()


def transformer_part(queries, attn_keys, attn_values, residual, out_weight, out_gate,
                     head_shift, head_scale, head_weight, head_bias):
    nx, nz = lax.axis_size("head"), lax.axis_size("seq") // 2
    frames, height, breadth, features = queries.shape
    model = residual.shape[3]
    rows, width = frames * height * breadth, features // nx
    heads = width // HEAD_DIM
    count = rows * nx
    planes = rows * nz
    share_cols = out_weight.shape[1]
    if nz != 2 * nx or heads != 3:
        raise ValueError("unsupported mesh")
    cells = head_weight.shape[1]
    there = pl.BlockSpec(memory_space=pltpu.HBM)
    vmem = pl.BlockSpec(memory_space=pltpu.VMEM)
    dma = pltpu.SemaphoreType.DMA
    bf, f32 = jnp.bfloat16, jnp.float32
    tile = 4 * share_cols
    return pl.pallas_call(
        functools.partial(block_kernel, nx, nz),
        out_shape=(jax.ShapeDtypeStruct((rows, model), bf), jax.ShapeDtypeStruct((2, 3, rows, 2 * cells), bf)),
        in_specs=[there] * 10,
        out_specs=(there, vmem),
        scratch_shapes=[
            pltpu.VMEM((count, HEAD_DIM), bf),
            pltpu.VMEM((2, nz, count, HEAD_DIM), bf),
            pltpu.VMEM((2, nz, count, HEAD_DIM), bf),
            pltpu.VMEM((planes, HEAD_DIM), bf),
            pltpu.VMEM((2, nx, planes, HEAD_DIM), bf),
            pltpu.VMEM((2, nx, planes, HEAD_DIM), bf),
            pltpu.VMEM((nz, 2, share_cols, width), bf),
            pltpu.VMEM((heads, HEAD_DIM, count), bf),
            pltpu.VMEM((heads, HEAD_DIM, count), f32),
            pltpu.VMEM((heads, 2, 1, count), f32),
            pltpu.VMEM((count, model), f32),
            pltpu.VMEM((nz // 2, nx, rows, tile), bf),
            pltpu.VMEM((nz // 2, nx, rows, tile), bf),
            pltpu.VMEM((count, width), bf),
            pltpu.VMEM((planes, HEAD_DIM), bf),
            pltpu.VMEM((rows, model), bf),
            pltpu.VMEM((2, 3, rows, 2 * cells), bf),
            pltpu.VMEM((rows, model), bf),
            pltpu.VMEM((1, model), f32),
            pltpu.VMEM((1, model), f32),
            pltpu.VMEM((1, model), f32),
            pltpu.VMEM((cells, model), bf),
            pltpu.VMEM((1, cells), f32),
            dma((13,)), dma((6,)), dma((6,)),
            dma((4, nz // 2 + 1)), dma((4, nz // 2 + 1)),
            dma((2, nz)), dma((2, nz)),
            dma((4, nx // 2 + 1)), dma((4, nx // 2 + 1)),
            dma((2, nx)), dma((2, nx)),
            dma((nz,)), dma((2 * nx,)),
            dma((2, nz // 2 + 1)), dma((2, nz // 2 + 1)),
            dma((nz,)), dma((nz,)),
            dma((nz // 2, nx)), dma((nz // 2, nx)),
            dma((5,)), dma((5,)), dma((1,)),
        ],
        compiler_params=pltpu.CompilerParams(
            collective_id=0, has_side_effects=True, vmem_limit_bytes=56 * 2**20),
        cost_estimate=pl.CostEstimate(flops=4 * count * count * 2 * nz * width, bytes_accessed=2**21, transcendentals=0),
        name="block_ring",
    )(queries.reshape(rows, features), attn_keys.reshape(rows, features), attn_values.reshape(rows, features),
      out_weight.T, residual.reshape(rows, model), out_gate.reshape(1, model), head_shift.reshape(1, model),
      head_scale.reshape(1, model), head_weight.T, head_bias.reshape(1, cells))


def on_device(queries, attn_keys, attn_values, residual, out_weight, out_gate, head_shift, head_scale,
              head_weight, head_bias, conv_weight, conv_bias, norm_gain):
    frames, height, breadth = queries.shape[:3]
    channels = head_weight.shape[1] // 4
    hidden, lat = transformer_part(queries, attn_keys, attn_values, residual, out_weight, out_gate,
                                   head_shift, head_scale, head_weight, head_bias)
    cells = lat[..., : 4 * channels].reshape(2, 3, frames, breadth, 2, 2, channels)
    video = cells.transpose(0, 2, 1, 4, 3, 5, 6).reshape(2 * frames, 6, 2 * breadth, channels)[:, 1:5]
    padded = jnp.pad(video, ((0, 0), (0, 0), (1, 1), (0, 0)))
    features = convolve(padded, frames, conv_weight, conv_bias, norm_gain)
    return hidden.reshape(residual.shape), features


def solution(mesh):
    return jax.shard_map(
        on_device,
        mesh=mesh,
        in_specs=(
            P(("clip", "head"), "seq", None, None),
            P(("clip", "head"), "seq", None, None),
            P(("clip", "head"), "seq", None, None),
            P(("clip", "head"), "seq", None, None),
            P("head", "seq"),
            P(),
            P(),
            P(),
            P(),
            P(),
            P(),
            P(),
            P(),
        ),
        out_specs=(P(("clip", "head"), "seq", None, None), P(("clip", "head"), "seq", None, None)),
        check_vma=False,
    )
```

```python
import functools

import jax
import jax.numpy as jnp
from jax import lax
from jax.experimental import pallas as pl
from jax.experimental.pallas import tpu as pltpu
from jax.sharding import PartitionSpec as P

HEAD_DIM = 128
MESH = pl.DeviceIdType.MESH


def convolve(padded, frames, conv_weight, conv_bias, norm_gain):
    height = padded.shape[1] - 2
    breadth = padded.shape[2] - 2
    stacked = jnp.concatenate(
        [
            padded[
                time_off : time_off + frames,
                row_off : row_off + height,
                col_off : col_off + breadth,
            ]
            for time_off in range(3)
            for row_off in range(3)
            for col_off in range(3)
        ],
        -1,
    )
    kernel = conv_weight.reshape(-1, conv_weight.shape[-1])
    linear = (
        jnp.dot(stacked.reshape(-1, stacked.shape[-1]), kernel, preferred_element_type=jnp.float32)
        + conv_bias
    )
    normed = linear * lax.rsqrt(jnp.mean(linear * linear, -1, keepdims=True) + 1e-06) * norm_gain
    return jax.nn.silu(normed).astype(jnp.bfloat16).reshape(frames, height, breadth, -1)


def block_kernel(nx, nz, q_in, k_in, v_in, w_in, res_in, gate_in, shift_in, scale_in, hw_in, hb_in,
                 hidden_ref, lat_ref,
                 qa, ka, va, qp, kp, vp, wbuf, qt, acc, stat, part, sums_out, sums_in, tokens, plane_out, owned, lat,
                 res, gate, shift, gain, hw, hb,
                 local_sem, a2a_send, a2a_recv, ring_send, ring_recv, pair_send, pair_recv,
                 pring_send, pring_recv, ppair_send, ppair_recv, back_send, back_recv,
                 w_send, w_recv, wpair_send, wpair_recv, rs_send, rs_recv, halo_send, halo_recv, out_sem):
    x = lax.axis_index("head")
    s = lax.axis_index("seq")
    z, c = s // 2, lax.rem(s, 2)
    nseq = 2 * nz
    rows, width = k_in.shape[0], tokens.shape[1]
    scale = HEAD_DIM ** (-0.5) * 1.4426950408889634
    halfz, halfx = nz // 2, nx // 2
    queries = qt.shape[2]

    def away(value, by, size):
        return lax.rem(value + by + 2 * size, size)

    def seq_of(zz, cc):
        return away(zz, 0, nz) * 2 + cc

    def remote(src, dst, send, recv, **where):
        return pltpu.make_async_remote_copy(
            src_ref=src, dst_ref=dst, send_sem=send, recv_sem=recv, device_id=where, device_id_type=MESH)

    def span(i, size):
        return pl.ds(pl.multiple_of(i * size, size), size)

    def column_head(xx):
        return span(xx * (width // HEAD_DIM), HEAD_DIM)

    def plane_head(zz):
        return span((zz // 2) * (width // HEAD_DIM) + 1 + lax.rem(zz, 2), HEAD_DIM)

    ins = (k_in, v_in, q_in)
    col_dst = (ka.at[c, z], va.at[c, z], qa)
    plane_dst = (kp.at[c, x], vp.at[c, x], qp)
    loads = [pltpu.make_async_copy(ins[i].at[:, column_head(x)], col_dst[i].at[span(x, rows), :], local_sem.at[i])
             for i in range(3)]
    loads += [pltpu.make_async_copy(ins[i].at[:, plane_head(z)], plane_dst[i].at[span(z, rows), :], local_sem.at[3 + i])
              for i in range(3)]
    w_load = pltpu.make_async_copy(w_in, wbuf.at[z, c], local_sem.at[6])
    late = ((res_in, res), (gate_in, gate), (shift_in, shift), (scale_in, gain), (hw_in, hw), (hb_in, hb))
    late = [pltpu.make_async_copy(a, b, local_sem.at[7 + i]) for i, (a, b) in enumerate(late)]
    for load in loads + [w_load] + late:
        load.start()
    lat[...] = jnp.zeros_like(lat)

    alone = (z // 2 == x).astype(jnp.int32)
    barrier = pltpu.get_barrier_semaphore()

    def greet(**where):
        pl.semaphore_signal(barrier, inc=1, device_id=where, device_id_type=MESH)

    for d in range(1, nx):
        greet(head=away(x, d, nx))
    for d in range(1, nz):
        greet(seq=seq_of(z + d, c))
    for other in (seq_of(z, 1 - c), away(s, 2 * c - 1, nseq)):
        greet(seq=other)
    for dx in (1, -1):
        for ds in (1, -1):
            greet(head=away(x, dx, nx), seq=away(s, ds, nseq))
    for xx in range(nx):
        for half in range(2):
            @pl.when(jnp.logical_or(x != xx, z != 2 * x + half))
            def _():
                greet(head=xx, seq=seq_of(2 * x + half, c))
    pl.semaphore_wait(barrier, nx - 1 + nz - 1 + 2 + 4 + 2 * nx - alone)

    def far_first(size):
        return sorted(range(1, size), key=lambda d: -min(d, size - d))

    def exchange(i):
        for d in far_first(nz):
            to = away(z, d, nz)
            remote(ins[i].at[:, plane_head(to)], plane_dst[i].at[span(z, rows), :],
                   a2a_send.at[3 + i], a2a_recv.at[3 + i], seq=seq_of(to, c)).start()
        for d in far_first(nx):
            to = away(x, d, nx)
            remote(ins[i].at[:, column_head(to)], col_dst[i].at[span(x, rows), :],
                   a2a_send.at[i], a2a_recv.at[i], head=to).start()

    for i in range(3):
        exchange(i)

    def from_column(i):
        piece = col_dst[i].at[pl.ds(0, rows * (nx - 1)), :]
        return remote(piece, piece, a2a_send.at[i], a2a_recv.at[i], head=away(x, 1, nx))

    def from_plane(i):
        piece = plane_dst[i].at[pl.ds(0, rows * (nz - 1)), :]
        return remote(piece, piece, a2a_send.at[3 + i], a2a_recv.at[3 + i], seq=seq_of(z + 1, c))

    col_kv, plane_kv = (ka, va), (kp, vp)

    def flow_of(kv, direction):
        return 2 * kv + (1 if direction > 0 else 0)

    def hop(kv, direction, step, back):
        slot, flow = col_kv[kv].at[c, away(z, -direction * back, nz)], flow_of(kv, direction)
        return remote(slot, slot, ring_send.at[flow, step], ring_recv.at[flow, step], seq=seq_of(z + direction, c))

    def share(kv, zz, cc):
        slot = col_kv[kv].at[cc, zz]
        return remote(slot, slot, pair_send.at[kv, zz], pair_recv.at[kv, zz], seq=seq_of(z, 1 - c))

    def phop(kv, direction, step, back):
        slot, flow = plane_kv[kv].at[c, away(x, -direction * back, nx)], flow_of(kv, direction)
        return remote(slot, slot, pring_send.at[flow, step], pring_recv.at[flow, step], head=away(x, direction, nx))

    def pshare(kv, xx, cc):
        slot = plane_kv[kv].at[cc, xx]
        return remote(slot, slot, ppair_send.at[kv, xx], ppair_recv.at[kv, xx], seq=seq_of(z, 1 - c))

    def w_hop(direction, step, back):
        slot, flow = wbuf.at[away(z, -direction * back, nz), c], 1 if direction > 0 else 0
        return remote(slot, slot, w_send.at[flow, step], w_recv.at[flow, step], seq=seq_of(z + direction, c))

    def w_share(zz, cc):
        slot = wbuf.at[zz, cc]
        return remote(slot, slot, wpair_send.at[zz], wpair_recv.at[zz], seq=seq_of(z, 1 - c))

    def last_hop(kv, direction, half):
        return half if (kv == 0) == (direction > 0) else half - 1

    def w_last(direction):
        return halfz if direction > 0 else halfz - 1

    def w_step(h):
        for direction in (1, -1):
            @pl.when(h <= w_last(direction))
            def _():
                w_hop(direction, h, h).wait_recv()

                @pl.when(h < w_last(direction))
                def _():
                    w_hop(direction, h + 1, h).start()

                w_share(away(z, -direction * h, nz), c).start()

    def col_step(h, kinds=(0, 1)):
        for kv in kinds:
            for direction in (1, -1):
                @pl.when(h <= last_hop(kv, direction, halfz))
                def _():
                    hop(kv, direction, h, h).wait_recv()

                    @pl.when(h < last_hop(kv, direction, halfz))
                    def _():
                        hop(kv, direction, h + 1, h).start()

                    share(kv, away(z, -direction * h, nz), c).start()

    def plane_step(h):
        for kv in range(2):
            for direction in (1, -1):
                @pl.when(h <= last_hop(kv, direction, halfx))
                def _():
                    phop(kv, direction, h, h).wait_recv()

                    @pl.when(h < last_hop(kv, direction, halfx))
                    def _():
                        phop(kv, direction, h + 1, h).start()

                    pshare(kv, away(x, -direction * h, nx), c).start()

    def fold(j, keys, values):
        scores = [lax.dot_general(key[...], qt[j], (((1,), (0,)), ((), ())), preferred_element_type=jnp.float32)
                  for key in keys]
        before = stat[j, 0]
        peak = before
        for part_scores in scores:
            peak = jnp.maximum(peak, jnp.max(part_scores, 0, keepdims=True))
        factor = jnp.exp2((before - peak) * scale)
        total, product = stat[j, 1] * factor, acc[j] * factor
        for part_scores, value in zip(scores, values):
            weights = jnp.exp2((part_scores - peak) * scale)
            total = total + jnp.sum(weights, 0, keepdims=True)
            product = product + lax.dot_general(value[...], weights.astype(jnp.bfloat16), (((0,), (0,)), ((), ())),
                                                preferred_element_type=jnp.float32)
        stat[j, 0], stat[j, 1], acc[j] = peak, total, product

    def col_attend(zs):
        for zz in zs:
            for kv in range(2):
                share(kv, zz, 1 - c).wait_recv()
        fold(0, [ka.at[lane, zz] for zz in zs for lane in range(2)], [va.at[lane, zz] for zz in zs for lane in range(2)])

    def col_attend_at(h):
        col_attend([away(z, -h, nz), away(z, h, nz)])

    def plane_attend(xx):
        for kv in range(2):
            pshare(kv, xx, 1 - c).wait_recv()

        for j in range(1, qt.shape[0]):
            fold(j, [kp.at[lane, xx] for lane in range(2)], [vp.at[lane, xx] for lane in range(2)])

    w_load.wait()
    for direction in (1, -1):
        w_hop(direction, 1, 0).start()
    w_share(z, c).start()
    for kv in range(2):
        loads[3 + kv].wait()
        from_plane(kv).wait_recv()
        for direction in (1, -1):
            if last_hop(kv, direction, halfx) >= 1:
                phop(kv, direction, 1, 0).start()
        pshare(kv, x, c).start()
    for kv in range(2):
        loads[kv].wait()
        from_column(kv).wait_recv()
        for direction in (1, -1):
            hop(kv, direction, 1, 0).start()
        share(kv, z, c).start()
    w_step(1)
    col_step(1)
    for i in (2, 5):
        loads[i].wait()
    from_column(2).wait_recv()
    from_plane(2).wait_recv()
    plane_step(1)

    acc[...] = jnp.zeros_like(acc)
    stat[:, 0] = jnp.full(stat[:, 0].shape, -1e30, jnp.float32)
    stat[:, 1] = jnp.zeros_like(stat[:, 1])
    qt[0] = qa[...].astype(jnp.float32).T.astype(jnp.bfloat16)
    for j in range(1, qt.shape[0]):
        qt[j] = qp[(j - 1) * queries:j * queries, :].astype(jnp.float32).T.astype(jnp.bfloat16)
    col_attend([z])
    plane_attend(x)
    w_step(2)
    w_at = [2]

    def w_reach(h):
        while w_at[0] < min(h, halfz):
            w_at[0] += 1
            w_step(w_at[0])

    def step(i, carry):
        col_step(2 * i, (0,))
        col_attend_at(2 * i - 1)
        col_step(2 * i, (1,))
        plane_attend(away(x, -i, nx))
        plane_step(i + 1)
        col_step(2 * i + 1, (0,))
        plane_attend(away(x, i, nx))
        col_step(2 * i + 1, (1,))
        col_attend_at(2 * i)
        return carry

    lax.fori_loop(1, halfx, step, 0)
    w_reach(3)
    plane_attend(away(x, halfx, nx))

    for j in range(1, qt.shape[0]):
        plane_out[(j - 1) * queries:j * queries, :] = (acc[j] / stat[j, 1]).T.astype(jnp.bfloat16)
    group, which = z // 2, lax.rem(z, 2)

    def back(zz, xx, part_of):
        return remote(plane_out.at[span(zz, rows), :], tokens.at[span(xx, rows), span(1 + part_of, HEAD_DIM)],
                      back_send.at[zz], back_recv.at[2 * xx + part_of], head=group, seq=seq_of(zz, c))

    for d in far_first(nz) + [0]:
        zz = away(z, d, nz)
        if d:
            back(zz, x, which).start()
        else:
            @pl.when(alone == 0)
            def _():
                back(zz, x, which).start()

            @pl.when(alone == 1)
            def _():
                tokens[span(x, rows), span(1 + which, HEAD_DIM)] = plane_out[span(zz, rows), :]

    col_step(halfz)
    col_attend_at(halfz - 1)
    w_reach(4)
    col_attend([away(z, halfz, nz)])
    tokens[:, 0:HEAD_DIM] = (acc[0] / stat[0, 1]).T.astype(jnp.bfloat16)
    w_reach(5)
    for xx in range(nx):
        for part_of in range(2):
            @pl.when(jnp.logical_or(alone == 0, jnp.logical_or(x != xx, which != part_of)))
            def _():
                back(z, xx, part_of).wait_recv()

    tile = 4 * w_in.shape[0]
    blocks = nz // 2
    order = sorted(range(1 - (blocks + 1) // 2, blocks // 2 + 1), key=lambda k: (abs(k), -k))
    flows = [(f, away(z // 2, k, blocks)) for f, k in enumerate(order)]
    groups = [flows[g:g + 2] for g in range(0, blocks, 2)]
    reach = [max(min(2 * abs(order[f]) + 1, halfz) for f, _ in group) for group in groups]

    def project(block):
        for i in range(2):
            w_share(2 * block + i, 1 - c).wait_recv()
        columns = wbuf[pl.ds(2 * block, 2)].reshape(tile, width)
        part[:, span(block, tile)] = lax.dot_general(
            tokens[...], columns, (((1,), (1,)), ((), ())), preferred_element_type=jnp.float32)

    def term(block, ahead):
        return part[span(away(x, ahead, nx), rows), span(block, tile)]

    sides = (1, -1)

    def hops(f, direction):
        return halfx if (f % 2 == 0) == (direction > 0) else halfx - 1

    def rs(f, direction, t):
        i = 2 * f + (1 if direction > 0 else 0)
        return remote(sums_out.at[i, t], sums_in.at[i, t], rs_send.at[i, t], rs_recv.at[i, t],
                      head=away(x, direction, nx))

    def advance(group, t):
        for direction in sides:
            for f, block in group:
                last = hops(f, direction)
                if t > last:
                    continue
                i = 2 * f + (1 if direction > 0 else 0)
                value = term(block, direction * (last - t + 1))
                if t > 1:
                    rs(f, direction, t - 1).wait_recv()
                    value = value + sums_in[i, t - 1].astype(jnp.float32)
                sums_out[i, t] = value.astype(jnp.bfloat16)
                rs(f, direction, t).start()

    def finish(group):
        for f, block in group:
            total = term(block, 0)
            for direction in sides:
                last = hops(f, direction)
                if last:
                    rs(f, direction, last).wait_recv()
                    total = total + sums_in[2 * f + (1 if direction > 0 else 0), last].astype(jnp.float32)
            at = span(block, tile)
            owned[:, at] = (res[:, at].astype(jnp.float32) + gate[:, at] * total).astype(jnp.bfloat16)

    entry = [max(0, g - 1) for g in range(len(groups))]
    for load in late:
        load.wait()
    for turn in range(halfx + 1 + entry[-1]):
        for g, group in enumerate(groups):
            t = turn - entry[g] + 1
            if t == 1:
                w_reach(reach[g])
                for f, block in group:
                    project(block)
            if 1 <= t <= halfx:
                advance(group, t)
            elif t == halfx + 1:
                finish(group)
        w_reach(6 + turn)

    out = pltpu.make_async_copy(owned, hidden_ref, out_sem.at[0])
    out.start()
    values = owned[...].astype(jnp.float32)
    center = values - jnp.mean(values, -1, keepdims=True)
    spread = jnp.mean(center * center, -1, keepdims=True)
    normed = (center * lax.rsqrt(spread + 1e-06) * (1.0 + gain[...]) + shift[...]).astype(jnp.bfloat16)
    latent = lax.dot_general(normed, hw[...], (((1,), (1,)), ((), ())), preferred_element_type=jnp.float32) + hb[...]
    cells = latent.shape[1]
    lat[1, 1, :, 0:cells] = latent.astype(jnp.bfloat16)

    sends = []
    for i, (dx, ds) in enumerate(((0, 1), (0, -1), (1, 0), (1, 1), (1, -1))):
        def copy(i=i, dx=dx, ds=ds):
            return remote(lat.at[1, 1], lat.at[1 - dx, 1 - ds], halo_send.at[i], halo_recv.at[i],
                          head=away(x, dx, nx), seq=away(s, ds, nseq))
        goes, comes = s >= 0, s >= 0
        if ds:
            goes = goes & (s + ds >= 0) & (s + ds < nseq)
            comes = comes & (s - ds >= 0) & (s - ds < nseq)
        if dx:
            goes = goes & (x + 1 < nx)
            comes = comes & (x > 0)
        sends.append((copy, goes, comes))
    for copy, goes, comes in sends:
        @pl.when(goes)
        def _():
            copy().start()

    for i in range(3):
        from_column(i).wait_send()
        from_plane(i).wait_send()

    def drain(h, carry):
        for kv in range(2):
            for direction in (1, -1):
                @pl.when(h <= last_hop(kv, direction, halfz))
                def _():
                    hop(kv, direction, h, h - 1).wait_send()

                @pl.when(h <= last_hop(kv, direction, halfx))
                def _():
                    phop(kv, direction, h, h - 1).wait_send()
        for direction in (1, -1):
            @pl.when(h <= w_last(direction))
            def _():
                w_hop(direction, h, h - 1).wait_send()
        return carry

    lax.fori_loop(1, halfz + 1, drain, 0)

    def drain_pair(zz, carry):
        for kv in range(2):
            share(kv, zz, c).wait_send()

            @pl.when(zz < nx)
            def _():
                pshare(kv, zz, c).wait_send()
        w_share(zz, c).wait_send()

        @pl.when(jnp.logical_or(alone == 0, zz != z))
        def _():
            back(zz, x, which).wait_send()
        return carry

    lax.fori_loop(0, nz, drain_pair, 0)

    for f, block in flows:
        for direction in sides:
            for t in range(1, hops(f, direction) + 1):
                rs(f, direction, t).wait_send()
    for copy, goes, comes in sends:
        @pl.when(comes)
        def _():
            copy().wait_recv()
    lat_ref[...] = lat[...]
    for copy, goes, comes in sends:
        @pl.when(goes)
        def _():
            copy().wait_send()
    out.wait()


def transformer_part(queries, attn_keys, attn_values, residual, out_weight, out_gate,
                     head_shift, head_scale, head_weight, head_bias):
    nx, nz = lax.axis_size("head"), lax.axis_size("seq") // 2
    frames, height, breadth, features = queries.shape
    model = residual.shape[3]
    rows, width = frames * height * breadth, features // nx
    heads = width // HEAD_DIM
    count = rows * nx
    planes = rows * nz
    share_cols = out_weight.shape[1]
    if nz != 2 * nx or heads != 3:
        raise ValueError("unsupported mesh")
    cells = head_weight.shape[1]
    there = pl.BlockSpec(memory_space=pltpu.HBM)
    vmem = pl.BlockSpec(memory_space=pltpu.VMEM)
    dma = pltpu.SemaphoreType.DMA
    bf, f32 = jnp.bfloat16, jnp.float32
    tile = 4 * share_cols
    return pl.pallas_call(
        functools.partial(block_kernel, nx, nz),
        out_shape=(jax.ShapeDtypeStruct((rows, model), bf), jax.ShapeDtypeStruct((2, 3, rows, 2 * cells), bf)),
        in_specs=[there] * 10,
        out_specs=(there, vmem),
        scratch_shapes=[
            pltpu.VMEM((count, HEAD_DIM), bf),
            pltpu.VMEM((2, nz, count, HEAD_DIM), bf),
            pltpu.VMEM((2, nz, count, HEAD_DIM), bf),
            pltpu.VMEM((planes, HEAD_DIM), bf),
            pltpu.VMEM((2, nx, planes, HEAD_DIM), bf),
            pltpu.VMEM((2, nx, planes, HEAD_DIM), bf),
            pltpu.VMEM((nz, 2, share_cols, width), bf),
            pltpu.VMEM((heads, HEAD_DIM, count), bf),
            pltpu.VMEM((heads, HEAD_DIM, count), f32),
            pltpu.VMEM((heads, 2, 1, count), f32),
            pltpu.VMEM((count, model), f32),
            pltpu.VMEM((nz, nx // 2 + 1, rows, tile), bf),
            pltpu.VMEM((nz, nx // 2 + 1, rows, tile), bf),
            pltpu.VMEM((count, width), bf),
            pltpu.VMEM((planes, HEAD_DIM), bf),
            pltpu.VMEM((rows, model), bf),
            pltpu.VMEM((2, 3, rows, 2 * cells), bf),
            pltpu.VMEM((rows, model), bf),
            pltpu.VMEM((1, model), f32),
            pltpu.VMEM((1, model), f32),
            pltpu.VMEM((1, model), f32),
            pltpu.VMEM((cells, model), bf),
            pltpu.VMEM((1, cells), f32),
            dma((13,)), dma((6,)), dma((6,)),
            dma((4, nz // 2 + 1)), dma((4, nz // 2 + 1)),
            dma((2, nz)), dma((2, nz)),
            dma((4, nx // 2 + 1)), dma((4, nx // 2 + 1)),
            dma((2, nx)), dma((2, nx)),
            dma((nz,)), dma((2 * nx,)),
            dma((2, nz // 2 + 1)), dma((2, nz // 2 + 1)),
            dma((nz,)), dma((nz,)),
            dma((nz, nx // 2 + 1)), dma((nz, nx // 2 + 1)),
            dma((5,)), dma((5,)), dma((1,)),
        ],
        compiler_params=pltpu.CompilerParams(
            collective_id=0, has_side_effects=True, vmem_limit_bytes=56 * 2**20),
        cost_estimate=pl.CostEstimate(flops=4 * count * count * 2 * nz * width, bytes_accessed=2**21, transcendentals=0),
        name="block_ring",
    )(queries.reshape(rows, features), attn_keys.reshape(rows, features), attn_values.reshape(rows, features),
      out_weight.T, residual.reshape(rows, model), out_gate.reshape(1, model), head_shift.reshape(1, model),
      head_scale.reshape(1, model), head_weight.T, head_bias.reshape(1, cells))


def on_device(queries, attn_keys, attn_values, residual, out_weight, out_gate, head_shift, head_scale,
              head_weight, head_bias, conv_weight, conv_bias, norm_gain):
    frames, height, breadth = queries.shape[:3]
    channels = head_weight.shape[1] // 4
    hidden, lat = transformer_part(queries, attn_keys, attn_values, residual, out_weight, out_gate,
                                   head_shift, head_scale, head_weight, head_bias)
    cells = lat[..., : 4 * channels].reshape(2, 3, frames, breadth, 2, 2, channels)
    video = cells.transpose(0, 2, 1, 4, 3, 5, 6).reshape(2 * frames, 6, 2 * breadth, channels)[:, 1:5]
    padded = jnp.pad(video, ((0, 0), (0, 0), (1, 1), (0, 0)))
    features = convolve(padded, frames, conv_weight, conv_bias, norm_gain)
    return hidden.reshape(residual.shape), features


def solution(mesh):
    return jax.shard_map(
        on_device,
        mesh=mesh,
        in_specs=(
            P(("clip", "head"), "seq", None, None),
            P(("clip", "head"), "seq", None, None),
            P(("clip", "head"), "seq", None, None),
            P(("clip", "head"), "seq", None, None),
            P("head", "seq"),
            P(),
            P(),
            P(),
            P(),
            P(),
            P(),
            P(),
            P(),
        ),
        out_specs=(P(("clip", "head"), "seq", None, None), P(("clip", "head"), "seq", None, None)),
        check_vma=False,
    )
```

```python
import functools

import jax
import jax.numpy as jnp
from jax import lax
from jax.experimental import pallas as pl
from jax.experimental.pallas import tpu as pltpu
from jax.sharding import PartitionSpec as P

HEAD_DIM = 128
MESH = pl.DeviceIdType.MESH


def block_kernel(nx, nz, frames, q_in, k_in, v_in, w_in, res_in, gate_in, shift_in, scale_in, hw_in, hb_in,
                 cw_in, cb_in, ng_in, owned, feat_ref,
                 qa, ka, va, qp, kp, vp, wbuf, qt, acc, stat, part, sums_out, sums_in, tokens, plane_out, lat, video, patches,
                 res, gate, shift, gain, hw, hb, cw, cb, ng,
                 local_sem, a2a_send, a2a_recv, ring_send, ring_recv, pair_send, pair_recv,
                 pring_send, pring_recv, ppair_send, ppair_recv, back_send, back_recv,
                 w_send, w_recv, wpair_send, wpair_recv, rs_send, rs_recv, halo_send, halo_recv):
    x = lax.axis_index("head")
    s = lax.axis_index("seq")
    z, c = s // 2, lax.rem(s, 2)
    nseq = 2 * nz
    rows, width = k_in.shape[0], tokens.shape[1]
    scale = HEAD_DIM ** (-0.5) * 1.4426950408889634
    halfz, halfx = nz // 2, nx // 2
    queries = qt.shape[2]

    def away(value, by, size):
        return lax.rem(value + by + 2 * size, size)

    def seq_of(zz, cc):
        return away(zz, 0, nz) * 2 + cc

    def remote(src, dst, send, recv, **where):
        return pltpu.make_async_remote_copy(
            src_ref=src, dst_ref=dst, send_sem=send, recv_sem=recv, device_id=where, device_id_type=MESH)

    def span(i, size):
        return pl.ds(pl.multiple_of(i * size, size), size)

    def column_head(xx):
        return span(xx * (width // HEAD_DIM), HEAD_DIM)

    def plane_head(zz):
        return span((zz // 2) * (width // HEAD_DIM) + 1 + lax.rem(zz, 2), HEAD_DIM)

    ins = (k_in, v_in, q_in)
    col_dst = (ka.at[c, z], va.at[c, z], qa)
    plane_dst = (kp.at[c, x], vp.at[c, x], qp)
    loads = [pltpu.make_async_copy(ins[i].at[:, column_head(x)], col_dst[i].at[span(x, rows), :], local_sem.at[i])
             for i in range(3)]
    loads += [pltpu.make_async_copy(ins[i].at[:, plane_head(z)], plane_dst[i].at[span(z, rows), :], local_sem.at[3 + i])
              for i in range(3)]
    w_load = pltpu.make_async_copy(w_in, wbuf.at[z, c], local_sem.at[6])
    late = ((res_in, res), (gate_in, gate), (shift_in, shift), (scale_in, gain), (hw_in, hw), (hb_in, hb),
            (cw_in, cw), (cb_in, cb), (ng_in, ng))
    late = [pltpu.make_async_copy(a, b, local_sem.at[7 + i]) for i, (a, b) in enumerate(late)]
    for load in loads + [w_load] + late:
        load.start()
    lat[...] = jnp.zeros_like(lat)
    video[...] = jnp.zeros_like(video)

    alone = (z // 2 == x).astype(jnp.int32)
    barrier = pltpu.get_barrier_semaphore()

    def greet(**where):
        pl.semaphore_signal(barrier, inc=1, device_id=where, device_id_type=MESH)

    for d in range(1, nx):
        greet(head=away(x, d, nx))
    for d in range(1, nz):
        greet(seq=seq_of(z + d, c))
    for other in (seq_of(z, 1 - c), away(s, 2 * c - 1, nseq)):
        greet(seq=other)
    for dx in (1, -1):
        for ds in (1, -1):
            greet(head=away(x, dx, nx), seq=away(s, ds, nseq))
    for xx in range(nx):
        for half in range(2):
            @pl.when(jnp.logical_or(x != xx, z != 2 * x + half))
            def _():
                greet(head=xx, seq=seq_of(2 * x + half, c))
    pl.semaphore_wait(barrier, nx - 1 + nz - 1 + 2 + 4 + 2 * nx - alone)

    def far_first(size):
        return sorted(range(1, size), key=lambda d: -min(d, size - d))

    def exchange(i):
        for d in far_first(nz):
            to = away(z, d, nz)
            remote(ins[i].at[:, plane_head(to)], plane_dst[i].at[span(z, rows), :],
                   a2a_send.at[3 + i], a2a_recv.at[3 + i], seq=seq_of(to, c)).start()
        for d in far_first(nx):
            to = away(x, d, nx)
            remote(ins[i].at[:, column_head(to)], col_dst[i].at[span(x, rows), :],
                   a2a_send.at[i], a2a_recv.at[i], head=to).start()

    for i in range(3):
        exchange(i)

    def from_column(i):
        piece = col_dst[i].at[pl.ds(0, rows * (nx - 1)), :]
        return remote(piece, piece, a2a_send.at[i], a2a_recv.at[i], head=away(x, 1, nx))

    def from_plane(i):
        piece = plane_dst[i].at[pl.ds(0, rows * (nz - 1)), :]
        return remote(piece, piece, a2a_send.at[3 + i], a2a_recv.at[3 + i], seq=seq_of(z + 1, c))

    col_kv, plane_kv = (ka, va), (kp, vp)

    def flow_of(kv, direction):
        return 2 * kv + (1 if direction > 0 else 0)

    def hop(kv, direction, step, back):
        slot, flow = col_kv[kv].at[c, away(z, -direction * back, nz)], flow_of(kv, direction)
        return remote(slot, slot, ring_send.at[flow, step], ring_recv.at[flow, step], seq=seq_of(z + direction, c))

    def share(kv, zz, cc):
        slot = col_kv[kv].at[cc, zz]
        return remote(slot, slot, pair_send.at[kv, zz], pair_recv.at[kv, zz], seq=seq_of(z, 1 - c))

    def phop(kv, direction, step, back):
        slot, flow = plane_kv[kv].at[c, away(x, -direction * back, nx)], flow_of(kv, direction)
        return remote(slot, slot, pring_send.at[flow, step], pring_recv.at[flow, step], head=away(x, direction, nx))

    def pshare(kv, xx, cc):
        slot = plane_kv[kv].at[cc, xx]
        return remote(slot, slot, ppair_send.at[kv, xx], ppair_recv.at[kv, xx], seq=seq_of(z, 1 - c))

    def w_hop(direction, step, back):
        slot, flow = wbuf.at[away(z, -direction * back, nz), c], 1 if direction > 0 else 0
        return remote(slot, slot, w_send.at[flow, step], w_recv.at[flow, step], seq=seq_of(z + direction, c))

    def w_share(zz, cc):
        slot = wbuf.at[zz, cc]
        return remote(slot, slot, wpair_send.at[zz], wpair_recv.at[zz], seq=seq_of(z, 1 - c))

    def last_hop(kv, direction, half):
        return half if (kv == 0) == (direction > 0) else half - 1

    def w_last(direction):
        return halfz if direction > 0 else halfz - 1

    def w_step(h):
        for direction in (1, -1):
            @pl.when(h <= w_last(direction))
            def _():
                w_hop(direction, h, h).wait_recv()

                @pl.when(h < w_last(direction))
                def _():
                    w_hop(direction, h + 1, h).start()

                w_share(away(z, -direction * h, nz), c).start()

    def col_step(h, kinds=(0, 1)):
        for kv in kinds:
            for direction in (1, -1):
                @pl.when(h <= last_hop(kv, direction, halfz))
                def _():
                    hop(kv, direction, h, h).wait_recv()

                    @pl.when(h < last_hop(kv, direction, halfz))
                    def _():
                        hop(kv, direction, h + 1, h).start()

                    share(kv, away(z, -direction * h, nz), c).start()

    def plane_step(h):
        for kv in range(2):
            for direction in (1, -1):
                @pl.when(h <= last_hop(kv, direction, halfx))
                def _():
                    phop(kv, direction, h, h).wait_recv()

                    @pl.when(h < last_hop(kv, direction, halfx))
                    def _():
                        phop(kv, direction, h + 1, h).start()

                    pshare(kv, away(x, -direction * h, nx), c).start()

    def fold(j, keys, values):
        scores = [lax.dot_general(key[...], qt[j], (((1,), (0,)), ((), ())), preferred_element_type=jnp.float32)
                  for key in keys]
        before = stat[j, 0]
        peak = before
        for part_scores in scores:
            peak = jnp.maximum(peak, jnp.max(part_scores, 0, keepdims=True))
        factor = jnp.exp2((before - peak) * scale)
        total, product = stat[j, 1] * factor, acc[j] * factor
        for part_scores, value in zip(scores, values):
            weights = jnp.exp2((part_scores - peak) * scale)
            total = total + jnp.sum(weights, 0, keepdims=True)
            product = product + lax.dot_general(value[...], weights.astype(jnp.bfloat16), (((0,), (0,)), ((), ())),
                                                preferred_element_type=jnp.float32)
        stat[j, 0], stat[j, 1], acc[j] = peak, total, product

    def col_attend(zs):
        for zz in zs:
            for kv in range(2):
                share(kv, zz, 1 - c).wait_recv()
        fold(0, [ka.at[lane, zz] for zz in zs for lane in range(2)], [va.at[lane, zz] for zz in zs for lane in range(2)])

    def col_attend_at(h):
        col_attend([away(z, -h, nz), away(z, h, nz)])

    def plane_attend(xx):
        for kv in range(2):
            pshare(kv, xx, 1 - c).wait_recv()

        for j in range(1, qt.shape[0]):
            fold(j, [kp.at[lane, xx] for lane in range(2)], [vp.at[lane, xx] for lane in range(2)])

    w_load.wait()
    for direction in (1, -1):
        w_hop(direction, 1, 0).start()
    w_share(z, c).start()
    for kv in range(2):
        loads[3 + kv].wait()
        from_plane(kv).wait_recv()
        for direction in (1, -1):
            if last_hop(kv, direction, halfx) >= 1:
                phop(kv, direction, 1, 0).start()
        pshare(kv, x, c).start()
    for kv in range(2):
        loads[kv].wait()
        from_column(kv).wait_recv()
        for direction in (1, -1):
            hop(kv, direction, 1, 0).start()
        share(kv, z, c).start()
    w_step(1)
    col_step(1)
    for i in (2, 5):
        loads[i].wait()
    from_column(2).wait_recv()
    from_plane(2).wait_recv()
    plane_step(1)

    acc[...] = jnp.zeros_like(acc)
    stat[:, 0] = jnp.full(stat[:, 0].shape, -1e30, jnp.float32)
    stat[:, 1] = jnp.zeros_like(stat[:, 1])
    qt[0] = qa[...].astype(jnp.float32).T.astype(jnp.bfloat16)
    for j in range(1, qt.shape[0]):
        qt[j] = qp[(j - 1) * queries:j * queries, :].astype(jnp.float32).T.astype(jnp.bfloat16)
    col_attend([z])
    plane_attend(x)
    w_step(2)
    w_at = [2]

    def w_reach(h):
        while w_at[0] < min(h, halfz):
            w_at[0] += 1
            w_step(w_at[0])

    def step(i, carry):
        col_step(2 * i, (0,))
        col_attend_at(2 * i - 1)
        col_step(2 * i, (1,))
        plane_attend(away(x, -i, nx))
        plane_step(i + 1)
        col_step(2 * i + 1, (0,))
        plane_attend(away(x, i, nx))
        col_step(2 * i + 1, (1,))
        col_attend_at(2 * i)
        if halfx > 2:
            @pl.when(i > halfx - 3)
            def _():
                w_step(i + 5 - halfx)
        return carry

    lax.fori_loop(1, halfx, step, 0)
    if halfx > 2:
        w_at[0] = 4
    w_reach(3)
    plane_attend(away(x, halfx, nx))

    for j in range(1, qt.shape[0]):
        plane_out[(j - 1) * queries:j * queries, :] = (acc[j] / stat[j, 1]).T.astype(jnp.bfloat16)
    group, which = z // 2, lax.rem(z, 2)

    def back(zz, xx, part_of):
        return remote(plane_out.at[span(zz, rows), :], tokens.at[span(xx, rows), span(1 + part_of, HEAD_DIM)],
                      back_send.at[zz], back_recv.at[2 * xx + part_of], head=group, seq=seq_of(zz, c))

    for d in far_first(nz) + [0]:
        zz = away(z, d, nz)
        if d:
            back(zz, x, which).start()
        else:
            @pl.when(alone == 0)
            def _():
                back(zz, x, which).start()

            @pl.when(alone == 1)
            def _():
                tokens[span(x, rows), span(1 + which, HEAD_DIM)] = plane_out[span(zz, rows), :]

    col_step(halfz)
    col_attend_at(halfz - 1)
    w_reach(5)
    col_attend([away(z, halfz, nz)])
    tokens[:, 0:HEAD_DIM] = (acc[0] / stat[0, 1]).T.astype(jnp.bfloat16)
    w_reach(6)
    for xx in range(nx):
        for part_of in range(2):
            @pl.when(jnp.logical_or(alone == 0, jnp.logical_or(x != xx, which != part_of)))
            def _():
                back(z, xx, part_of).wait_recv()

    tile = 4 * w_in.shape[0]
    blocks = nz // 2
    order = sorted(range(1 - (blocks + 1) // 2, blocks // 2 + 1), key=lambda k: (abs(k), -k))
    flows = [(f, away(z // 2, k, blocks)) for f, k in enumerate(order)]
    groups = [flows[g:g + 2] for g in range(0, blocks, 2)]
    reach = [max(min(2 * abs(order[f]) + 1, halfz) for f, _ in group) for group in groups]

    def project(block):
        for i in range(2):
            w_share(2 * block + i, 1 - c).wait_recv()
        columns = wbuf[pl.ds(2 * block, 2)].reshape(tile, width)
        part[:, span(block, tile)] = lax.dot_general(
            tokens[...], columns, (((1,), (1,)), ((), ())), preferred_element_type=jnp.float32)

    def term(block, ahead):
        return part[span(away(x, ahead, nx), rows), span(block, tile)]

    sides = (1, -1)

    def hops(f, direction):
        return halfx if (f % 2 == 0) == (direction > 0) else halfx - 1

    def rs(f, direction, t):
        i = 2 * f + (1 if direction > 0 else 0)
        return remote(sums_out.at[i, t], sums_in.at[i, t], rs_send.at[i, t], rs_recv.at[i, t],
                      head=away(x, direction, nx))

    def advance(group, t):
        for direction in sides:
            for f, block in group:
                last = hops(f, direction)
                if t > last:
                    continue
                i = 2 * f + (1 if direction > 0 else 0)
                value = term(block, direction * (last - t + 1))
                if t > 1:
                    rs(f, direction, t - 1).wait_recv()
                    value = value + sums_in[i, t - 1].astype(jnp.float32)
                sums_out[i, t] = value.astype(jnp.bfloat16)
                rs(f, direction, t).start()

    def finish(group):
        for f, block in group:
            total = term(block, 0)
            for direction in sides:
                last = hops(f, direction)
                if last:
                    rs(f, direction, last).wait_recv()
                    total = total + sums_in[2 * f + (1 if direction > 0 else 0), last].astype(jnp.float32)
            at = span(block, tile)
            owned[:, at] = (res[:, at].astype(jnp.float32) + gate[:, at] * total).astype(jnp.bfloat16)

    entry = [g // 2 for g in range(len(groups))]
    for load in late:
        load.wait()
    for turn in range(halfx + 1 + entry[-1]):
        for g, group in enumerate(groups):
            t = turn - entry[g] + 1
            if t == 1:
                w_reach(reach[g])
                for f, block in group:
                    project(block)
            if 1 <= t <= halfx:
                advance(group, t)
            elif t == halfx + 1:
                finish(group)
        w_reach(7 + turn)

    values = owned[...].astype(jnp.float32)
    center = values - jnp.mean(values, -1, keepdims=True)
    spread = jnp.mean(center * center, -1, keepdims=True)
    normed = (center * lax.rsqrt(spread + 1e-06) * (1.0 + gain[...]) + shift[...]).astype(jnp.bfloat16)
    latent = lax.dot_general(normed, hw[...], (((1,), (1,)), ((), ())), preferred_element_type=jnp.float32) + hb[...]
    cells = latent.shape[1]
    lat[1, 1, :, 0:cells] = latent.astype(jnp.bfloat16)

    sends = []
    for i, (dx, ds) in enumerate(((0, 1), (0, -1), (1, 0), (1, 1), (1, -1))):
        def copy(i=i, dx=dx, ds=ds):
            return remote(lat.at[1, 1], lat.at[1 - dx, 1 - ds], halo_send.at[i], halo_recv.at[i],
                          head=away(x, dx, nx), seq=away(s, ds, nseq))
        goes, comes = s >= 0, s >= 0
        if ds:
            goes = goes & (s + ds >= 0) & (s + ds < nseq)
            comes = comes & (s - ds >= 0) & (s - ds < nseq)
        if dx:
            goes = goes & (x + 1 < nx)
            comes = comes & (x > 0)
        sends.append((copy, goes, comes))
    for copy, goes, comes in sends:
        @pl.when(goes)
        def _():
            copy().start()

    for i in range(3):
        from_column(i).wait_send()
        from_plane(i).wait_send()

    def drain(h, carry):
        for kv in range(2):
            for direction in (1, -1):
                @pl.when(h <= last_hop(kv, direction, halfz))
                def _():
                    hop(kv, direction, h, h - 1).wait_send()

                @pl.when(h <= last_hop(kv, direction, halfx))
                def _():
                    phop(kv, direction, h, h - 1).wait_send()
        for direction in (1, -1):
            @pl.when(h <= w_last(direction))
            def _():
                w_hop(direction, h, h - 1).wait_send()
        return carry

    lax.fori_loop(1, halfz + 1, drain, 0)

    def drain_pair(zz, carry):
        for kv in range(2):
            share(kv, zz, c).wait_send()

            @pl.when(zz < nx)
            def _():
                pshare(kv, zz, c).wait_send()
        w_share(zz, c).wait_send()

        @pl.when(jnp.logical_or(alone == 0, zz != z))
        def _():
            back(zz, x, which).wait_send()
        return carry

    lax.fori_loop(0, nz, drain_pair, 0)

    for f, block in flows:
        for direction in sides:
            for t in range(1, hops(f, direction) + 1):
                rs(f, direction, t).wait_send()
    for copy, goes, comes in sends:
        @pl.when(comes)
        def _():
            copy().wait_recv()
    channels, breadth = cells // 4, rows // frames
    for group_of in range(2):
        for frame in range(frames):
            here = slice(frame * breadth, (frame + 1) * breadth)
            for line, (row, a) in enumerate(((0, 1), (1, 0), (1, 1), (2, 0))):
                for b in range(2):
                    at = (2 * a + b) * channels
                    video[group_of * frames + frame, line, pl.ds(1 + b, breadth, stride=2), :] = (
                        lat[group_of, row, here, at:at + channels].astype(jnp.float32))
    for k in range(27):
        dt, dy, dx = k // 9, k // 3 % 3, k % 3
        for frame in range(frames):
            for line in range(2):
                at = (2 * frame + line) * 2 * breadth
                patches[at:at + 2 * breadth, k * channels:(k + 1) * channels] = (
                    video[frame + dt, line + dy, dx:dx + 2 * breadth, :])
    linear = jnp.dot(patches[...].astype(jnp.bfloat16), cw[...], preferred_element_type=jnp.float32) + cb[...]
    level = lax.rsqrt(jnp.mean(linear * linear, -1, keepdims=True) + 1e-06)
    gated = linear * level * ng[...]
    feat_ref[...] = (gated / (1.0 + jnp.exp(-gated))).astype(feat_ref.dtype)
    for copy, goes, comes in sends:
        @pl.when(goes)
        def _():
            copy().wait_send()


def transformer_part(queries, attn_keys, attn_values, residual, out_weight, out_gate,
                     head_shift, head_scale, head_weight, head_bias, conv_weight, conv_bias, norm_gain):
    nx, nz = lax.axis_size("head"), lax.axis_size("seq") // 2
    frames, height, breadth, features = queries.shape
    model = residual.shape[3]
    rows, width = frames * height * breadth, features // nx
    heads = width // HEAD_DIM
    count = rows * nx
    planes = rows * nz
    share_cols = out_weight.shape[1]
    if nz != 2 * nx or heads != 3:
        raise ValueError("unsupported mesh")
    cells = head_weight.shape[1]
    taps, outs = conv_weight.size // conv_weight.shape[-1], conv_weight.shape[-1]
    places = 4 * rows
    if frames != 2 or conv_weight.shape[:3] != (3, 3, 3) or height != 1:
        raise ValueError("unsupported shape")
    there = pl.BlockSpec(memory_space=pltpu.HBM)
    vmem = pl.BlockSpec(memory_space=pltpu.VMEM)
    dma = pltpu.SemaphoreType.DMA
    bf, f32 = jnp.bfloat16, jnp.float32
    tile = 4 * share_cols
    return pl.pallas_call(
        functools.partial(block_kernel, nx, nz, frames),
        out_shape=(jax.ShapeDtypeStruct((rows, model), bf), jax.ShapeDtypeStruct((places, outs), bf)),
        in_specs=[there] * 13,
        out_specs=(vmem, vmem),
        scratch_shapes=[
            pltpu.VMEM((count, HEAD_DIM), bf),
            pltpu.VMEM((2, nz, count, HEAD_DIM), bf),
            pltpu.VMEM((2, nz, count, HEAD_DIM), bf),
            pltpu.VMEM((planes, HEAD_DIM), bf),
            pltpu.VMEM((2, nx, planes, HEAD_DIM), bf),
            pltpu.VMEM((2, nx, planes, HEAD_DIM), bf),
            pltpu.VMEM((nz, 2, share_cols, width), bf),
            pltpu.VMEM((heads, HEAD_DIM, count), bf),
            pltpu.VMEM((heads, HEAD_DIM, count), f32),
            pltpu.VMEM((heads, 2, 1, count), f32),
            pltpu.VMEM((count, model), f32),
            pltpu.VMEM((nz, nx // 2 + 1, rows, tile), bf),
            pltpu.VMEM((nz, nx // 2 + 1, rows, tile), bf),
            pltpu.VMEM((count, width), bf),
            pltpu.VMEM((planes, HEAD_DIM), bf),
            pltpu.VMEM((2, 3, rows, 2 * cells), bf),
            pltpu.VMEM((2 * frames, 4, 2 * breadth + 8, cells // 4), f32),
            pltpu.VMEM((places, taps), f32),
            pltpu.VMEM((rows, model), bf),
            pltpu.VMEM((1, model), f32),
            pltpu.VMEM((1, model), f32),
            pltpu.VMEM((1, model), f32),
            pltpu.VMEM((cells, model), bf),
            pltpu.VMEM((1, cells), f32),
            pltpu.VMEM((taps, outs), bf),
            pltpu.VMEM((1, outs), f32),
            pltpu.VMEM((1, outs), f32),
            dma((16,)), dma((6,)), dma((6,)),
            dma((4, nz // 2 + 1)), dma((4, nz // 2 + 1)),
            dma((2, nz)), dma((2, nz)),
            dma((4, nx // 2 + 1)), dma((4, nx // 2 + 1)),
            dma((2, nx)), dma((2, nx)),
            dma((nz,)), dma((2 * nx,)),
            dma((2, nz // 2 + 1)), dma((2, nz // 2 + 1)),
            dma((nz,)), dma((nz,)),
            dma((nz, nx // 2 + 1)), dma((nz, nx // 2 + 1)),
            dma((5,)), dma((5,)),
        ],
        compiler_params=pltpu.CompilerParams(
            collective_id=0, has_side_effects=True, vmem_limit_bytes=56 * 2**20),
        cost_estimate=pl.CostEstimate(flops=4 * count * count * 2 * nz * width, bytes_accessed=2**21, transcendentals=0),
        name="block_ring",
    )(queries.reshape(rows, features), attn_keys.reshape(rows, features), attn_values.reshape(rows, features),
      out_weight.T, residual.reshape(rows, model), out_gate.reshape(1, model), head_shift.reshape(1, model),
      head_scale.reshape(1, model), head_weight.T, head_bias.reshape(1, cells),
      conv_weight.reshape(taps, outs), conv_bias.reshape(1, outs), norm_gain.reshape(1, outs))


def on_device(queries, attn_keys, attn_values, residual, out_weight, out_gate, head_shift, head_scale,
              head_weight, head_bias, conv_weight, conv_bias, norm_gain):
    frames, height, breadth = queries.shape[:3]
    hidden, features = transformer_part(queries, attn_keys, attn_values, residual, out_weight, out_gate, head_shift,
                                        head_scale, head_weight, head_bias, conv_weight, conv_bias, norm_gain)
    return hidden.reshape(residual.shape), features.reshape(frames, 2 * height, 2 * breadth, -1)


def solution(mesh):
    return jax.shard_map(
        on_device,
        mesh=mesh,
        in_specs=(
            P(("clip", "head"), "seq", None, None),
            P(("clip", "head"), "seq", None, None),
            P(("clip", "head"), "seq", None, None),
            P(("clip", "head"), "seq", None, None),
            P("head", "seq"),
            P(),
            P(),
            P(),
            P(),
            P(),
            P(),
            P(),
            P(),
        ),
        out_specs=(P(("clip", "head"), "seq", None, None), P(("clip", "head"), "seq", None, None)),
        check_vma=False,
    )
```

```python
import functools

import jax
import jax.numpy as jnp
from jax import lax
from jax.experimental import pallas as pl
from jax.experimental.pallas import tpu as pltpu
from jax.sharding import PartitionSpec as P

HEAD_DIM = 128
MESH = pl.DeviceIdType.MESH


def block_kernel(nx, nz, frames, q_in, k_in, v_in, w_in, res_in, gate_in, shift_in, scale_in, hw_in, hb_in,
                 cw_in, cb_in, ng_in, hidden_ref, feat_ref,
                 qa, ka, va, qp, kp, vp, wbuf, qt, acc, stat, part, sums_out, sums_in, tokens, plane_out, owned, feat, lat, video, patches,
                 res, gate, shift, gain, hw, hb, cw, cb, ng,
                 local_sem, a2a_send, a2a_recv, ring_send, ring_recv, pair_send, pair_recv,
                 pring_send, pring_recv, ppair_send, ppair_recv, back_send, back_recv,
                 w_send, w_recv, wpair_send, wpair_recv, rs_send, rs_recv, halo_send, halo_recv, out_sem):
    x = lax.axis_index("head")
    s = lax.axis_index("seq")
    z, c = s // 2, lax.rem(s, 2)
    nseq = 2 * nz
    rows, width = k_in.shape[0], tokens.shape[1]
    scale = HEAD_DIM ** (-0.5) * 1.4426950408889634
    halfz, halfx = nz // 2, nx // 2
    queries = qt.shape[2]

    def away(value, by, size):
        return lax.rem(value + by + 2 * size, size)

    def seq_of(zz, cc):
        return away(zz, 0, nz) * 2 + cc

    def remote(src, dst, send, recv, **where):
        return pltpu.make_async_remote_copy(
            src_ref=src, dst_ref=dst, send_sem=send, recv_sem=recv, device_id=where, device_id_type=MESH)

    def span(i, size):
        return pl.ds(pl.multiple_of(i * size, size), size)

    def column_head(xx):
        return span(xx * (width // HEAD_DIM), HEAD_DIM)

    def plane_head(zz):
        return span((zz // 2) * (width // HEAD_DIM) + 1 + lax.rem(zz, 2), HEAD_DIM)

    ins = (k_in, v_in, q_in)
    col_dst = (ka.at[c, z], va.at[c, z], qa)
    plane_dst = (kp.at[c, x], vp.at[c, x], qp)
    loads = [pltpu.make_async_copy(ins[i].at[:, column_head(x)], col_dst[i].at[span(x, rows), :], local_sem.at[i])
             for i in range(3)]
    loads += [pltpu.make_async_copy(ins[i].at[:, plane_head(z)], plane_dst[i].at[span(z, rows), :], local_sem.at[3 + i])
              for i in range(3)]
    w_load = pltpu.make_async_copy(w_in, wbuf.at[z, c], local_sem.at[6])
    late = ((res_in, res), (gate_in, gate), (shift_in, shift), (scale_in, gain), (hw_in, hw), (hb_in, hb),
            (cw_in, cw), (cb_in, cb), (ng_in, ng))
    late = [pltpu.make_async_copy(a, b, local_sem.at[7 + i]) for i, (a, b) in enumerate(late)]
    for load in loads + [w_load] + late:
        load.start()
    lat[...] = jnp.zeros_like(lat)
    video[...] = jnp.zeros_like(video)

    alone = (z // 2 == x).astype(jnp.int32)
    barrier = pltpu.get_barrier_semaphore()

    def greet(**where):
        pl.semaphore_signal(barrier, inc=1, device_id=where, device_id_type=MESH)

    for d in range(1, nx):
        greet(head=away(x, d, nx))
    for d in range(1, nz):
        greet(seq=seq_of(z + d, c))
    for other in (seq_of(z, 1 - c), away(s, 2 * c - 1, nseq)):
        greet(seq=other)
    for dx in (1, -1):
        for ds in (1, -1):
            greet(head=away(x, dx, nx), seq=away(s, ds, nseq))
    for xx in range(nx):
        for half in range(2):
            @pl.when(jnp.logical_or(x != xx, z != 2 * x + half))
            def _():
                greet(head=xx, seq=seq_of(2 * x + half, c))
    pl.semaphore_wait(barrier, nx - 1 + nz - 1 + 2 + 4 + 2 * nx - alone)

    def far_first(size):
        return sorted(range(1, size), key=lambda d: -min(d, size - d))

    def exchange(i):
        for d in far_first(nz):
            to = away(z, d, nz)
            remote(ins[i].at[:, plane_head(to)], plane_dst[i].at[span(z, rows), :],
                   a2a_send.at[3 + i], a2a_recv.at[3 + i], seq=seq_of(to, c)).start()
        for d in far_first(nx):
            to = away(x, d, nx)
            remote(ins[i].at[:, column_head(to)], col_dst[i].at[span(x, rows), :],
                   a2a_send.at[i], a2a_recv.at[i], head=to).start()

    for i in range(3):
        exchange(i)

    def from_column(i):
        piece = col_dst[i].at[pl.ds(0, rows * (nx - 1)), :]
        return remote(piece, piece, a2a_send.at[i], a2a_recv.at[i], head=away(x, 1, nx))

    def from_plane(i):
        piece = plane_dst[i].at[pl.ds(0, rows * (nz - 1)), :]
        return remote(piece, piece, a2a_send.at[3 + i], a2a_recv.at[3 + i], seq=seq_of(z + 1, c))

    col_kv, plane_kv = (ka, va), (kp, vp)

    def flow_of(kv, direction):
        return 2 * kv + (1 if direction > 0 else 0)

    def hop(kv, direction, step, back):
        slot, flow = col_kv[kv].at[c, away(z, -direction * back, nz)], flow_of(kv, direction)
        return remote(slot, slot, ring_send.at[kv], ring_recv.at[flow, step - 1], seq=seq_of(z + direction, c))

    def share(kv, zz, cc):
        slot = col_kv[kv].at[cc, zz]
        return remote(slot, slot, pair_send.at[kv], pair_recv.at[kv, zz], seq=seq_of(z, 1 - c))

    def phop(kv, direction, step, back):
        slot, flow = plane_kv[kv].at[c, away(x, -direction * back, nx)], flow_of(kv, direction)
        return remote(slot, slot, pring_send.at[kv], pring_recv.at[flow, step - 1], head=away(x, direction, nx))

    def pshare(kv, xx, cc):
        slot = plane_kv[kv].at[cc, xx]
        return remote(slot, slot, ppair_send.at[kv], ppair_recv.at[kv, xx], seq=seq_of(z, 1 - c))

    def w_hop(direction, step, back):
        slot, flow = wbuf.at[away(z, -direction * back, nz), c], 1 if direction > 0 else 0
        return remote(slot, slot, w_send.at[0], w_recv.at[flow, step - 1], seq=seq_of(z + direction, c))

    def w_share(zz, cc):
        slot = wbuf.at[zz, cc]
        return remote(slot, slot, wpair_send.at[0], wpair_recv.at[zz], seq=seq_of(z, 1 - c))

    def last_hop(kv, direction, half):
        return half if (kv == 0) == (direction > 0) else half - 1

    def w_last(direction):
        return halfz if direction > 0 else halfz - 1

    def w_step(h):
        for direction in (1, -1):
            @pl.when(h <= w_last(direction))
            def _():
                w_hop(direction, h, h).wait_recv()

                @pl.when(h < w_last(direction))
                def _():
                    w_hop(direction, h + 1, h).start()

                w_share(away(z, -direction * h, nz), c).start()

    def col_step(h, kinds=(0, 1)):
        for kv in kinds:
            for direction in (1, -1):
                @pl.when(h <= last_hop(kv, direction, halfz))
                def _():
                    hop(kv, direction, h, h).wait_recv()

                    @pl.when(h < last_hop(kv, direction, halfz))
                    def _():
                        hop(kv, direction, h + 1, h).start()

                    share(kv, away(z, -direction * h, nz), c).start()

    def plane_step(h):
        for kv in range(2):
            for direction in (1, -1):
                @pl.when(h <= last_hop(kv, direction, halfx))
                def _():
                    phop(kv, direction, h, h).wait_recv()

                    @pl.when(h < last_hop(kv, direction, halfx))
                    def _():
                        phop(kv, direction, h + 1, h).start()

                    pshare(kv, away(x, -direction * h, nx), c).start()

    def fold(j, keys, values):
        scores = [lax.dot_general(key[...], qt[j], (((1,), (0,)), ((), ())), preferred_element_type=jnp.float32)
                  for key in keys]
        before = stat[j, 0]
        peak = before
        for part_scores in scores:
            peak = jnp.maximum(peak, jnp.max(part_scores, 0, keepdims=True))
        factor = jnp.exp2((before - peak) * scale)
        total, product = stat[j, 1] * factor, acc[j] * factor
        for part_scores, value in zip(scores, values):
            weights = jnp.exp2((part_scores - peak) * scale)
            total = total + jnp.sum(weights, 0, keepdims=True)
            product = product + lax.dot_general(value[...], weights.astype(jnp.bfloat16), (((0,), (0,)), ((), ())),
                                                preferred_element_type=jnp.float32)
        stat[j, 0], stat[j, 1], acc[j] = peak, total, product

    def col_attend(zs):
        for zz in zs:
            for kv in range(2):
                share(kv, zz, 1 - c).wait_recv()
        fold(0, [ka.at[lane, zz] for zz in zs for lane in range(2)], [va.at[lane, zz] for zz in zs for lane in range(2)])

    def col_attend_at(h):
        col_attend([away(z, -h, nz), away(z, h, nz)])

    def plane_attend(xx):
        for kv in range(2):
            pshare(kv, xx, 1 - c).wait_recv()

        for j in range(1, qt.shape[0]):
            fold(j, [kp.at[lane, xx] for lane in range(2)], [vp.at[lane, xx] for lane in range(2)])

    w_load.wait()
    for direction in (1, -1):
        w_hop(direction, 1, 0).start()
    w_share(z, c).start()
    for kv in range(2):
        loads[3 + kv].wait()
        from_plane(kv).wait_recv()
        for direction in (1, -1):
            if last_hop(kv, direction, halfx) >= 1:
                phop(kv, direction, 1, 0).start()
        pshare(kv, x, c).start()
    for kv in range(2):
        loads[kv].wait()
        from_column(kv).wait_recv()
        for direction in (1, -1):
            hop(kv, direction, 1, 0).start()
        share(kv, z, c).start()
    w_step(1)
    col_step(1)
    for i in (2, 5):
        loads[i].wait()
    from_column(2).wait_recv()
    from_plane(2).wait_recv()
    plane_step(1)

    acc[...] = jnp.zeros_like(acc)
    stat[:, 0] = jnp.full(stat[:, 0].shape, -1e30, jnp.float32)
    stat[:, 1] = jnp.zeros_like(stat[:, 1])
    qt[0] = qa[...].astype(jnp.float32).T.astype(jnp.bfloat16)
    for j in range(1, qt.shape[0]):
        qt[j] = qp[(j - 1) * queries:j * queries, :].astype(jnp.float32).T.astype(jnp.bfloat16)
    col_attend([z])
    plane_attend(x)
    w_step(2)
    w_at = [2]

    def w_reach(h):
        while w_at[0] < min(h, halfz):
            w_at[0] += 1
            w_step(w_at[0])

    def step(i, carry):
        col_step(2 * i, (0,))
        col_attend_at(2 * i - 1)
        col_step(2 * i, (1,))
        plane_attend(away(x, -i, nx))
        plane_step(i + 1)
        col_step(2 * i + 1, (0,))
        plane_attend(away(x, i, nx))
        col_step(2 * i + 1, (1,))
        col_attend_at(2 * i)
        if halfx > 2:
            @pl.when(i > halfx - 3)
            def _():
                w_step(i + 5 - halfx)
        return carry

    lax.fori_loop(1, halfx, step, 0)
    if halfx > 2:
        w_at[0] = 4
    w_reach(3)
    plane_attend(away(x, halfx, nx))

    for j in range(1, qt.shape[0]):
        plane_out[(j - 1) * queries:j * queries, :] = (acc[j] / stat[j, 1]).T.astype(jnp.bfloat16)
    group, which = z // 2, lax.rem(z, 2)

    def back(zz, xx, part_of):
        return remote(plane_out.at[span(zz, rows), :], tokens.at[span(xx, rows), span(1 + part_of, HEAD_DIM)],
                      back_send.at[0], back_recv.at[2 * xx + part_of], head=group, seq=seq_of(zz, c))

    for d in far_first(nz) + [0]:
        zz = away(z, d, nz)
        if d:
            back(zz, x, which).start()
        else:
            @pl.when(alone == 0)
            def _():
                back(zz, x, which).start()

            @pl.when(alone == 1)
            def _():
                tokens[span(x, rows), span(1 + which, HEAD_DIM)] = plane_out[span(zz, rows), :]

    col_step(halfz)
    col_attend_at(halfz - 1)
    w_reach(5)
    col_attend([away(z, halfz, nz)])
    tokens[:, 0:HEAD_DIM] = (acc[0] / stat[0, 1]).T.astype(jnp.bfloat16)
    w_reach(6)
    for xx in range(nx):
        for part_of in range(2):
            @pl.when(jnp.logical_or(alone == 0, jnp.logical_or(x != xx, which != part_of)))
            def _():
                back(z, xx, part_of).wait_recv()

    tile = 4 * w_in.shape[0]
    blocks = nz // 2
    order = sorted(range(1 - (blocks + 1) // 2, blocks // 2 + 1), key=lambda k: (abs(k), -k))
    flows = [(f, away(z // 2, k, blocks)) for f, k in enumerate(order)]
    groups = [flows[g:g + 2] for g in range(0, blocks, 2)]
    reach = [max(min(2 * abs(order[f]) + 1, halfz) for f, _ in group) for group in groups]

    def project(block):
        for i in range(2):
            w_share(2 * block + i, 1 - c).wait_recv()
        columns = wbuf[pl.ds(2 * block, 2)].reshape(tile, width)
        part[:, span(block, tile)] = lax.dot_general(
            tokens[...], columns, (((1,), (1,)), ((), ())), preferred_element_type=jnp.float32)

    def term(block, ahead):
        return part[span(away(x, ahead, nx), rows), span(block, tile)]

    sides = (1, -1)

    def hops(f, direction):
        return halfx if (f % 2 == 0) == (direction > 0) else halfx - 1

    def slot_of(f, direction, t):
        return f * (nx - 1) + (0 if direction > 0 else hops(f, 1)) + t - 1

    def rs(f, direction, t):
        i = slot_of(f, direction, t)
        return remote(sums_out.at[i], sums_in.at[i], rs_send.at[0], rs_recv.at[i], head=away(x, direction, nx))

    def advance(group, t):
        for direction in sides:
            for f, block in group:
                last = hops(f, direction)
                if t > last:
                    continue
                value = term(block, direction * (last - t + 1))
                if t > 1:
                    rs(f, direction, t - 1).wait_recv()
                    value = value + sums_in[slot_of(f, direction, t - 1)].astype(jnp.float32)
                sums_out[slot_of(f, direction, t)] = value.astype(jnp.bfloat16)
                rs(f, direction, t).start()

    def finish(group):
        for f, block in group:
            total = term(block, 0)
            for direction in sides:
                last = hops(f, direction)
                if last:
                    rs(f, direction, last).wait_recv()
                    total = total + sums_in[slot_of(f, direction, last)].astype(jnp.float32)
            at = span(block, tile)
            owned[:, at] = (res[:, at].astype(jnp.float32) + gate[:, at] * total).astype(jnp.bfloat16)

    entry = [g // 2 for g in range(len(groups))]
    for load in late:
        load.wait()
    for turn in range(halfx + 1 + entry[-1]):
        for g, group in enumerate(groups):
            t = turn - entry[g] + 1
            if t == 1:
                w_reach(reach[g])
                for f, block in group:
                    project(block)
            if 1 <= t <= halfx:
                advance(group, t)
            elif t == halfx + 1:
                finish(group)
        w_reach(7 + turn)

    out = pltpu.make_async_copy(owned, hidden_ref, out_sem.at[0])
    out.start()
    values = owned[...].astype(jnp.float32)
    center = values - jnp.mean(values, -1, keepdims=True)
    spread = jnp.mean(center * center, -1, keepdims=True)
    normed = (center * lax.rsqrt(spread + 1e-06) * (1.0 + gain[...]) + shift[...]).astype(jnp.bfloat16)
    latent = lax.dot_general(normed, hw[...], (((1,), (1,)), ((), ())), preferred_element_type=jnp.float32) + hb[...]
    cells = latent.shape[1]
    lat[1, 1, :, 0:cells] = latent.astype(jnp.bfloat16)

    sends = []
    for i, (dx, ds) in enumerate(((0, 1), (0, -1), (1, 0), (1, 1), (1, -1))):
        def copy(i=i, dx=dx, ds=ds):
            return remote(lat.at[1, 1], lat.at[1 - dx, 1 - ds], halo_send.at[i], halo_recv.at[i],
                          head=away(x, dx, nx), seq=away(s, ds, nseq))
        goes, comes = s >= 0, s >= 0
        if ds:
            goes = goes & (s + ds >= 0) & (s + ds < nseq)
            comes = comes & (s - ds >= 0) & (s - ds < nseq)
        if dx:
            goes = goes & (x + 1 < nx)
            comes = comes & (x > 0)
        sends.append((copy, goes, comes))
    for copy, goes, comes in sends:
        @pl.when(goes)
        def _():
            copy().start()

    for i in range(3):
        from_column(i).wait_send()
        from_plane(i).wait_send()

    def sent(ref, sem):
        remote(ref, ref, sem, sem, head=away(x, 1, nx)).wait_send()

    for kv in range(2):
        sent(col_kv[kv].at[0, pl.ds(0, nz - 1)], ring_send.at[kv])
        sent(col_kv[kv].at[0], pair_send.at[kv])
        sent(plane_kv[kv].at[0, pl.ds(0, nx - 1)], pring_send.at[kv])
        sent(plane_kv[kv].at[0], ppair_send.at[kv])
    sent(wbuf.at[pl.ds(0, nz - 1), 0], w_send.at[0])
    sent(wbuf.at[:, 0], wpair_send.at[0])
    sent(sums_out, rs_send.at[0])

    @pl.when(alone == 0)
    def _():
        sent(plane_out, back_send.at[0])

    @pl.when(alone == 1)
    def _():
        sent(plane_out.at[pl.ds(0, rows * (nz - 1)), :], back_send.at[0])

    for copy, goes, comes in sends:
        @pl.when(comes)
        def _():
            copy().wait_recv()
    channels, breadth = cells // 4, rows // frames
    for group_of in range(2):
        for frame in range(frames):
            here = slice(frame * breadth, (frame + 1) * breadth)
            for line, (row, a) in enumerate(((0, 1), (1, 0), (1, 1), (2, 0))):
                for b in range(2):
                    at = (2 * a + b) * channels
                    video[group_of * frames + frame, line, pl.ds(1 + b, breadth, stride=2), :] = (
                        lat[group_of, row, here, at:at + channels].astype(jnp.float32))
    for k in range(27):
        dt, dy, dx = k // 9, k // 3 % 3, k % 3
        for frame in range(frames):
            for line in range(2):
                at = (2 * frame + line) * 2 * breadth
                patches[at:at + 2 * breadth, k * channels:(k + 1) * channels] = (
                    video[frame + dt, line + dy, dx:dx + 2 * breadth, :])
    linear = jnp.dot(patches[...].astype(jnp.bfloat16), cw[...], preferred_element_type=jnp.float32) + cb[...][None, :]
    level = lax.rsqrt(jnp.mean(linear * linear, -1, keepdims=True) + 1e-06)
    gated = linear * level * ng[...][None, :]
    feat[...] = (gated / (1.0 + jnp.exp(-gated))).astype(feat.dtype)
    feat_out = pltpu.make_async_copy(feat, feat_ref, out_sem.at[1])
    feat_out.start()
    for copy, goes, comes in sends:
        @pl.when(goes)
        def _():
            copy().wait_send()
    out.wait()
    feat_out.wait()


def transformer_part(queries, attn_keys, attn_values, residual, out_weight, out_gate,
                     head_shift, head_scale, head_weight, head_bias, conv_weight, conv_bias, norm_gain):
    nx, nz = lax.axis_size("head"), lax.axis_size("seq") // 2
    frames, height, breadth, features = queries.shape
    model = residual.shape[3]
    rows, width = frames * height * breadth, features // nx
    heads = width // HEAD_DIM
    count = rows * nx
    planes = rows * nz
    share_cols = out_weight.shape[1]
    if nz != 2 * nx or heads != 3:
        raise ValueError("unsupported mesh")
    cells = head_weight.shape[1]
    taps, outs = conv_weight.size // conv_weight.shape[-1], conv_weight.shape[-1]
    places = 4 * rows
    if frames != 2 or conv_weight.shape[:3] != (3, 3, 3) or height != 1:
        raise ValueError("unsupported shape")
    there = pl.BlockSpec(memory_space=pltpu.HBM)
    dma = pltpu.SemaphoreType.DMA
    bf, f32 = jnp.bfloat16, jnp.float32
    tile = 4 * share_cols
    return pl.pallas_call(
        functools.partial(block_kernel, nx, nz, frames),
        out_shape=(jax.ShapeDtypeStruct((rows, model), bf), jax.ShapeDtypeStruct((places, outs), bf)),
        in_specs=[there] * 13,
        out_specs=(there, there),
        scratch_shapes=[
            pltpu.VMEM((count, HEAD_DIM), bf),
            pltpu.VMEM((2, nz, count, HEAD_DIM), bf),
            pltpu.VMEM((2, nz, count, HEAD_DIM), bf),
            pltpu.VMEM((planes, HEAD_DIM), bf),
            pltpu.VMEM((2, nx, planes, HEAD_DIM), bf),
            pltpu.VMEM((2, nx, planes, HEAD_DIM), bf),
            pltpu.VMEM((nz, 2, share_cols, width), bf),
            pltpu.VMEM((heads, HEAD_DIM, count), bf),
            pltpu.VMEM((heads, HEAD_DIM, count), f32),
            pltpu.VMEM((heads, 2, 1, count), f32),
            pltpu.VMEM((count, model), f32),
            pltpu.VMEM((nz // 2 * (nx - 1), rows, tile), bf),
            pltpu.VMEM((nz // 2 * (nx - 1), rows, tile), bf),
            pltpu.VMEM((count, width), bf),
            pltpu.VMEM((planes, HEAD_DIM), bf),
            pltpu.VMEM((rows, model), bf),
            pltpu.VMEM((places, outs), bf),
            pltpu.VMEM((2, 3, rows, 2 * cells), bf),
            pltpu.VMEM((2 * frames, 4, 2 * breadth + 8, cells // 4), f32),
            pltpu.VMEM((places, taps), f32),
            pltpu.VMEM((rows, model), bf),
            pltpu.VMEM((1, model), f32),
            pltpu.VMEM((1, model), f32),
            pltpu.VMEM((1, model), f32),
            pltpu.VMEM((cells, model), bf),
            pltpu.VMEM((1, cells), f32),
            pltpu.VMEM((taps, outs), bf),
            pltpu.VMEM((outs,), f32),
            pltpu.VMEM((outs,), f32),
            dma((16,)), dma((6,)), dma((6,)),
            dma((2,)), dma((4, nz // 2)), dma((2,)), dma((2, nz)),
            dma((2,)), dma((4, nx // 2)), dma((2,)), dma((2, nx)),
            dma((1,)), dma((2 * nx,)),
            dma((1,)), dma((2, nz // 2)), dma((1,)), dma((nz,)),
            dma((1,)), dma((nz // 2 * (nx - 1),)),
            dma((5,)), dma((5,)), dma((2,)),
        ],
        compiler_params=pltpu.CompilerParams(
            collective_id=0, has_side_effects=True, vmem_limit_bytes=56 * 2**20),
        cost_estimate=pl.CostEstimate(flops=4 * count * count * 2 * nz * width, bytes_accessed=2**21, transcendentals=0),
        name="block_ring",
    )(queries.reshape(rows, features), attn_keys.reshape(rows, features), attn_values.reshape(rows, features),
      out_weight.T, residual.reshape(rows, model), out_gate.reshape(1, model), head_shift.reshape(1, model),
      head_scale.reshape(1, model), head_weight.T, head_bias.reshape(1, cells),
      conv_weight.reshape(taps, outs), conv_bias, norm_gain)


def deliver_kernel(a_ref, b_ref, a_out, b_out, sem):
    copies = [pltpu.make_async_copy(a_ref, a_out, sem.at[0]), pltpu.make_async_copy(b_ref, b_out, sem.at[1])]
    for copy in copies:
        copy.start()
    for copy in copies:
        copy.wait()


def deliver(a, b):
    return pl.pallas_call(
        deliver_kernel,
        out_shape=(jax.ShapeDtypeStruct(a.shape, a.dtype), jax.ShapeDtypeStruct(b.shape, b.dtype)),
        in_specs=[pl.BlockSpec(memory_space=pltpu.VMEM)] * 2,
        out_specs=[pl.BlockSpec(memory_space=pltpu.HBM)] * 2,
        scratch_shapes=[pltpu.SemaphoreType.DMA((2,))],
        name="deliver",
    )(a, b)


def on_device(queries, attn_keys, attn_values, residual, out_weight, out_gate, head_shift, head_scale,
              head_weight, head_bias, conv_weight, conv_bias, norm_gain):
    frames, height, breadth = queries.shape[:3]
    hidden, features = transformer_part(queries, attn_keys, attn_values, residual, out_weight, out_gate, head_shift,
                                        head_scale, head_weight, head_bias, conv_weight, conv_bias, norm_gain)
    hidden, features = deliver(hidden, features)
    return hidden.reshape(residual.shape), features.reshape(frames, 2 * height, 2 * breadth, -1)


def solution(mesh):
    return jax.shard_map(
        on_device,
        mesh=mesh,
        in_specs=(
            P(("clip", "head"), "seq", None, None),
            P(("clip", "head"), "seq", None, None),
            P(("clip", "head"), "seq", None, None),
            P(("clip", "head"), "seq", None, None),
            P("head", "seq"),
            P(),
            P(),
            P(),
            P(),
            P(),
            P(),
            P(),
            P(),
        ),
        out_specs=(P(("clip", "head"), "seq", None, None), P(("clip", "head"), "seq", None, None)),
        check_vma=False,
    )
```

```python
import functools

import jax
import jax.numpy as jnp
from jax import lax
from jax.experimental import pallas as pl
from jax.experimental.pallas import tpu as pltpu
from jax.sharding import PartitionSpec as P

HEAD_DIM = 128
MESH = pl.DeviceIdType.MESH


def block_kernel(nx, nz, frames, q_in, k_in, v_in, w_in, res_in, gate_in, shift_in, scale_in, hw_in, hb_in,
                 cw_in, cb_in, ng_in, hidden_ref, feat_ref,
                 qa, ka, va, qp, kp, vp, wbuf, qt, acc, stat, part, sums_out, sums_in, tokens, plane_out, owned, feat, lat, video, patches,
                 res, gate, shift, gain, hw, hb, cw, cb, ng,
                 local_sem, a2a_send, a2a_recv, ring_send, ring_recv, pair_send, pair_recv,
                 pring_send, pring_recv, ppair_send, ppair_recv, back_send, back_recv,
                 w_send, w_recv, wpair_send, wpair_recv, rs_send, rs_recv, halo_send, halo_recv, out_sem):
    x = lax.axis_index("head")
    s = lax.axis_index("seq")
    z, c = s // 2, lax.rem(s, 2)
    nseq = 2 * nz
    rows, width = k_in.shape[0], tokens.shape[1]
    scale = HEAD_DIM ** (-0.5) * 1.4426950408889634
    halfz, halfx = nz // 2, nx // 2
    queries = qt.shape[2]

    def away(value, by, size):
        return lax.rem(value + by + 2 * size, size)

    def seq_of(zz, cc):
        return away(zz, 0, nz) * 2 + cc

    def remote(src, dst, send, recv, **where):
        return pltpu.make_async_remote_copy(
            src_ref=src, dst_ref=dst, send_sem=send, recv_sem=recv, device_id=where, device_id_type=MESH)

    def span(i, size):
        return pl.ds(pl.multiple_of(i * size, size), size)

    def column_head(xx):
        return span(xx * (width // HEAD_DIM), HEAD_DIM)

    def plane_head(zz):
        return span((zz // 2) * (width // HEAD_DIM) + 1 + lax.rem(zz, 2), HEAD_DIM)

    ins = (k_in, v_in, q_in)
    col_dst = (ka.at[c, z], va.at[c, z], qa)
    plane_dst = (kp.at[c, x], vp.at[c, x], qp)
    loads = [pltpu.make_async_copy(ins[i].at[:, column_head(x)], col_dst[i].at[span(x, rows), :], local_sem.at[i])
             for i in range(3)]
    loads += [pltpu.make_async_copy(ins[i].at[:, plane_head(z)], plane_dst[i].at[span(z, rows), :], local_sem.at[3 + i])
              for i in range(3)]
    w_load = pltpu.make_async_copy(w_in, wbuf.at[z, c], local_sem.at[6])
    late = ((res_in, res), (gate_in, gate), (shift_in, shift), (scale_in, gain), (hw_in, hw), (hb_in, hb),
            (cw_in, cw), (cb_in, cb), (ng_in, ng))
    late = [pltpu.make_async_copy(a, b, local_sem.at[7 + i]) for i, (a, b) in enumerate(late)]
    for load in loads + [w_load] + late:
        load.start()
    lat[...] = jnp.zeros_like(lat)
    video[...] = jnp.zeros_like(video)

    alone = (z // 2 == x).astype(jnp.int32)
    barrier = pltpu.get_barrier_semaphore()

    def greet(**where):
        pl.semaphore_signal(barrier, inc=1, device_id=where, device_id_type=MESH)

    for d in range(1, nx):
        greet(head=away(x, d, nx))
    for d in range(1, nz):
        greet(seq=seq_of(z + d, c))
    for other in (seq_of(z, 1 - c), away(s, 2 * c - 1, nseq)):
        greet(seq=other)
    for dx in (1, -1):
        for ds in (1, -1):
            greet(head=away(x, dx, nx), seq=away(s, ds, nseq))
    for xx in range(nx):
        for half in range(2):
            @pl.when(jnp.logical_or(x != xx, z != 2 * x + half))
            def _():
                greet(head=xx, seq=seq_of(2 * x + half, c))
    pl.semaphore_wait(barrier, nx - 1 + nz - 1 + 2 + 4 + 2 * nx - alone)

    def far_first(size):
        return sorted(range(1, size), key=lambda d: -min(d, size - d))

    def exchange(i):
        for d in far_first(nz):
            to = away(z, d, nz)
            remote(ins[i].at[:, plane_head(to)], plane_dst[i].at[span(z, rows), :],
                   a2a_send.at[3 + i], a2a_recv.at[3 + i], seq=seq_of(to, c)).start()
        for d in far_first(nx):
            to = away(x, d, nx)
            remote(ins[i].at[:, column_head(to)], col_dst[i].at[span(x, rows), :],
                   a2a_send.at[i], a2a_recv.at[i], head=to).start()

    for i in range(3):
        exchange(i)

    def from_column(i):
        piece = col_dst[i].at[pl.ds(0, rows * (nx - 1)), :]
        return remote(piece, piece, a2a_send.at[i], a2a_recv.at[i], head=away(x, 1, nx))

    def from_plane(i):
        piece = plane_dst[i].at[pl.ds(0, rows * (nz - 1)), :]
        return remote(piece, piece, a2a_send.at[3 + i], a2a_recv.at[3 + i], seq=seq_of(z + 1, c))

    col_kv, plane_kv = (ka, va), (kp, vp)

    def flow_of(kv, direction):
        return 2 * kv + (1 if direction > 0 else 0)

    def hop(kv, direction, step, back):
        slot, flow = col_kv[kv].at[c, away(z, -direction * back, nz)], flow_of(kv, direction)
        return remote(slot, slot, ring_send.at[kv], ring_recv.at[flow, step - 1], seq=seq_of(z + direction, c))

    def share(kv, zz, cc):
        slot = col_kv[kv].at[cc, zz]
        return remote(slot, slot, pair_send.at[kv], pair_recv.at[kv, zz], seq=seq_of(z, 1 - c))

    def phop(kv, direction, step, back):
        slot, flow = plane_kv[kv].at[c, away(x, -direction * back, nx)], flow_of(kv, direction)
        return remote(slot, slot, pring_send.at[kv], pring_recv.at[flow, step - 1], head=away(x, direction, nx))

    def pshare(kv, xx, cc):
        slot = plane_kv[kv].at[cc, xx]
        return remote(slot, slot, ppair_send.at[kv], ppair_recv.at[kv, xx], seq=seq_of(z, 1 - c))

    def w_hop(direction, step, back):
        slot, flow = wbuf.at[away(z, -direction * back, nz), c], 1 if direction > 0 else 0
        return remote(slot, slot, w_send.at[0], w_recv.at[flow, step - 1], seq=seq_of(z + direction, c))

    def w_share(zz, cc):
        slot = wbuf.at[zz, cc]
        return remote(slot, slot, wpair_send.at[0], wpair_recv.at[zz], seq=seq_of(z, 1 - c))

    def last_hop(kv, direction, half):
        return half if (kv == 0) == (direction > 0) else half - 1

    def w_last(direction):
        return halfz if direction > 0 else halfz - 1

    def w_step(h):
        for direction in (1, -1):
            @pl.when(h <= w_last(direction))
            def _():
                w_hop(direction, h, h).wait_recv()

                @pl.when(h < w_last(direction))
                def _():
                    w_hop(direction, h + 1, h).start()

                w_share(away(z, -direction * h, nz), c).start()

    def col_step(h, kinds=(0, 1)):
        for kv in kinds:
            for direction in (1, -1):
                @pl.when(h <= last_hop(kv, direction, halfz))
                def _():
                    hop(kv, direction, h, h).wait_recv()

                    @pl.when(h < last_hop(kv, direction, halfz))
                    def _():
                        hop(kv, direction, h + 1, h).start()

                    share(kv, away(z, -direction * h, nz), c).start()

    def plane_step(h):
        for kv in range(2):
            for direction in (1, -1):
                @pl.when(h <= last_hop(kv, direction, halfx))
                def _():
                    phop(kv, direction, h, h).wait_recv()

                    @pl.when(h < last_hop(kv, direction, halfx))
                    def _():
                        phop(kv, direction, h + 1, h).start()

                    pshare(kv, away(x, -direction * h, nx), c).start()

    def fold(j, keys, values):
        scores = [lax.dot_general(key[...], qt[j], (((1,), (0,)), ((), ())), preferred_element_type=jnp.float32)
                  for key in keys]
        before = stat[j, 0]
        peak = before
        for part_scores in scores:
            peak = jnp.maximum(peak, jnp.max(part_scores, 0, keepdims=True))
        factor = jnp.exp2((before - peak) * scale)
        total, product = stat[j, 1] * factor, acc[j] * factor
        for part_scores, value in zip(scores, values):
            weights = jnp.exp2((part_scores - peak) * scale)
            total = total + jnp.sum(weights, 0, keepdims=True)
            product = product + lax.dot_general(value[...], weights.astype(jnp.bfloat16), (((0,), (0,)), ((), ())),
                                                preferred_element_type=jnp.float32)
        stat[j, 0], stat[j, 1], acc[j] = peak, total, product

    def col_attend(zs):
        for zz in zs:
            for kv in range(2):
                share(kv, zz, 1 - c).wait_recv()
        fold(0, [ka.at[lane, zz] for zz in zs for lane in range(2)], [va.at[lane, zz] for zz in zs for lane in range(2)])

    def col_attend_at(h):
        col_attend([away(z, -h, nz), away(z, h, nz)])

    def plane_attend(xx):
        for kv in range(2):
            pshare(kv, xx, 1 - c).wait_recv()

        for j in range(1, qt.shape[0]):
            fold(j, [kp.at[lane, xx] for lane in range(2)], [vp.at[lane, xx] for lane in range(2)])

    w_load.wait()
    for direction in (1, -1):
        w_hop(direction, 1, 0).start()
    w_share(z, c).start()
    for kv in range(2):
        loads[3 + kv].wait()
        from_plane(kv).wait_recv()
        for direction in (1, -1):
            if last_hop(kv, direction, halfx) >= 1:
                phop(kv, direction, 1, 0).start()
        pshare(kv, x, c).start()
    for kv in range(2):
        loads[kv].wait()
        from_column(kv).wait_recv()
        for direction in (1, -1):
            hop(kv, direction, 1, 0).start()
        share(kv, z, c).start()
    w_step(1)
    col_step(1)
    for i in (2, 5):
        loads[i].wait()
    from_column(2).wait_recv()
    from_plane(2).wait_recv()
    plane_step(1)

    acc[...] = jnp.zeros_like(acc)
    stat[:, 0] = jnp.full(stat[:, 0].shape, -1e30, jnp.float32)
    stat[:, 1] = jnp.zeros_like(stat[:, 1])
    qt[0] = qa[...].astype(jnp.float32).T.astype(jnp.bfloat16)
    for j in range(1, qt.shape[0]):
        qt[j] = qp[(j - 1) * queries:j * queries, :].astype(jnp.float32).T.astype(jnp.bfloat16)
    col_attend([z])
    plane_attend(x)
    w_step(2)
    w_at = [2]

    def w_reach(h):
        while w_at[0] < min(h, halfz):
            w_at[0] += 1
            w_step(w_at[0])

    def step(i, carry):
        col_step(2 * i, (0,))
        col_attend_at(2 * i - 1)
        col_step(2 * i, (1,))
        plane_attend(away(x, -i, nx))
        plane_step(i + 1)
        col_step(2 * i + 1, (0,))
        plane_attend(away(x, i, nx))
        col_step(2 * i + 1, (1,))
        col_attend_at(2 * i)
        w_step(i + 2)
        return carry

    lax.fori_loop(1, halfx, step, 0)
    w_at[0] = max(2, halfx + 1)
    w_reach(3)
    plane_attend(away(x, halfx, nx))

    for j in range(1, qt.shape[0]):
        plane_out[(j - 1) * queries:j * queries, :] = (acc[j] / stat[j, 1]).T.astype(jnp.bfloat16)
    group, which = z // 2, lax.rem(z, 2)

    def back(zz, xx, part_of):
        return remote(plane_out.at[span(zz, rows), :], tokens.at[span(xx, rows), span(1 + part_of, HEAD_DIM)],
                      back_send.at[0], back_recv.at[2 * xx + part_of], head=group, seq=seq_of(zz, c))

    for d in far_first(nz) + [0]:
        zz = away(z, d, nz)
        if d:
            back(zz, x, which).start()
        else:
            @pl.when(alone == 0)
            def _():
                back(zz, x, which).start()

            @pl.when(alone == 1)
            def _():
                tokens[span(x, rows), span(1 + which, HEAD_DIM)] = plane_out[span(zz, rows), :]

    col_step(halfz)
    col_attend_at(halfz - 1)
    w_reach(6)
    col_attend([away(z, halfz, nz)])
    tokens[:, 0:HEAD_DIM] = (acc[0] / stat[0, 1]).T.astype(jnp.bfloat16)
    w_reach(7)
    for xx in range(nx):
        for part_of in range(2):
            @pl.when(jnp.logical_or(alone == 0, jnp.logical_or(x != xx, which != part_of)))
            def _():
                back(z, xx, part_of).wait_recv()

    tile = 4 * w_in.shape[0]
    blocks = nz // 2
    order = sorted(range(1 - (blocks + 1) // 2, blocks // 2 + 1), key=lambda k: (abs(k), -k))
    flows = [(f, away(z // 2, k, blocks)) for f, k in enumerate(order)]
    groups = [flows[g:g + 2] for g in range(0, blocks, 2)]
    reach = [max(min(2 * abs(order[f]) + 1, halfz) for f, _ in group) for group in groups]

    def project(block):
        for i in range(2):
            w_share(2 * block + i, 1 - c).wait_recv()
        columns = wbuf[pl.ds(2 * block, 2)].reshape(tile, width)
        part[:, span(block, tile)] = lax.dot_general(
            tokens[...], columns, (((1,), (1,)), ((), ())), preferred_element_type=jnp.float32)

    def term(block, ahead):
        return part[span(away(x, ahead, nx), rows), span(block, tile)]

    sides = (1, -1)

    def hops(f, direction):
        return halfx if (f % 2 == 0) == (direction > 0) else halfx - 1

    def slot_of(f, direction, t):
        return f * (nx - 1) + (0 if direction > 0 else hops(f, 1)) + t - 1

    def rs(f, direction, t):
        i = slot_of(f, direction, t)
        return remote(sums_out.at[i], sums_in.at[i], rs_send.at[0], rs_recv.at[i], head=away(x, direction, nx))

    def advance(group, t):
        for direction in sides:
            for f, block in group:
                last = hops(f, direction)
                if t > last:
                    continue
                value = term(block, direction * (last - t + 1))
                if t > 1:
                    rs(f, direction, t - 1).wait_recv()
                    value = value + sums_in[slot_of(f, direction, t - 1)].astype(jnp.float32)
                sums_out[slot_of(f, direction, t)] = value.astype(jnp.bfloat16)
                rs(f, direction, t).start()

    def finish(group):
        for f, block in group:
            total = term(block, 0)
            for direction in sides:
                last = hops(f, direction)
                if last:
                    rs(f, direction, last).wait_recv()
                    total = total + sums_in[slot_of(f, direction, last)].astype(jnp.float32)
            at = span(block, tile)
            owned[:, at] = (res[:, at].astype(jnp.float32) + gate[:, at] * total).astype(jnp.bfloat16)

    entry = [max(0, g - 2) for g in range(len(groups))]
    for load in late:
        load.wait()
    for turn in range(halfx + 1 + entry[-1]):
        for g, group in enumerate(groups):
            t = turn - entry[g] + 1
            if t == 1:
                w_reach(reach[g])
                for f, block in group:
                    project(block)
            if 1 <= t <= halfx:
                advance(group, t)
            elif t == halfx + 1:
                finish(group)
        w_reach(8 + turn)

    out = pltpu.make_async_copy(owned, hidden_ref, out_sem.at[0])
    out.start()
    values = owned[...].astype(jnp.float32)
    center = values - jnp.mean(values, -1, keepdims=True)
    spread = jnp.mean(center * center, -1, keepdims=True)
    normed = (center * lax.rsqrt(spread + 1e-06) * (1.0 + gain[...]) + shift[...]).astype(jnp.bfloat16)
    latent = lax.dot_general(normed, hw[...], (((1,), (1,)), ((), ())), preferred_element_type=jnp.float32) + hb[...]
    cells = latent.shape[1]
    lat[1, 1, :, 0:cells] = latent.astype(jnp.bfloat16)

    sends = []
    for i, (dx, ds) in enumerate(((0, 1), (0, -1), (1, 0), (1, 1), (1, -1))):
        def copy(i=i, dx=dx, ds=ds):
            return remote(lat.at[1, 1], lat.at[1 - dx, 1 - ds], halo_send.at[i], halo_recv.at[i],
                          head=away(x, dx, nx), seq=away(s, ds, nseq))
        goes, comes = s >= 0, s >= 0
        if ds:
            goes = goes & (s + ds >= 0) & (s + ds < nseq)
            comes = comes & (s - ds >= 0) & (s - ds < nseq)
        if dx:
            goes = goes & (x + 1 < nx)
            comes = comes & (x > 0)
        sends.append((copy, goes, comes))
    for copy, goes, comes in sends:
        @pl.when(goes)
        def _():
            copy().start()

    for i in range(3):
        from_column(i).wait_send()
        from_plane(i).wait_send()

    def sent(ref, sem):
        remote(ref, ref, sem, sem, head=away(x, 1, nx)).wait_send()

    for kv in range(2):
        sent(col_kv[kv].at[0, pl.ds(0, nz - 1)], ring_send.at[kv])
        sent(col_kv[kv].at[0], pair_send.at[kv])
        sent(plane_kv[kv].at[0, pl.ds(0, nx - 1)], pring_send.at[kv])
        sent(plane_kv[kv].at[0], ppair_send.at[kv])
    sent(wbuf.at[pl.ds(0, nz - 1), 0], w_send.at[0])
    sent(wbuf.at[:, 0], wpair_send.at[0])
    sent(sums_out, rs_send.at[0])

    @pl.when(alone == 0)
    def _():
        sent(plane_out, back_send.at[0])

    @pl.when(alone == 1)
    def _():
        sent(plane_out.at[pl.ds(0, rows * (nz - 1)), :], back_send.at[0])

    for copy, goes, comes in sends:
        @pl.when(comes)
        def _():
            copy().wait_recv()
    channels, breadth = cells // 4, rows // frames
    for group_of in range(2):
        for frame in range(frames):
            here = slice(frame * breadth, (frame + 1) * breadth)
            for line, (row, a) in enumerate(((0, 1), (1, 0), (1, 1), (2, 0))):
                for b in range(2):
                    at = (2 * a + b) * channels
                    video[group_of * frames + frame, line, pl.ds(1 + b, breadth, stride=2), :] = (
                        lat[group_of, row, here, at:at + channels].astype(jnp.float32))
    for k in range(27):
        dt, dy, dx = k // 9, k // 3 % 3, k % 3
        for frame in range(frames):
            for line in range(2):
                at = (2 * frame + line) * 2 * breadth
                patches[at:at + 2 * breadth, k * channels:(k + 1) * channels] = (
                    video[frame + dt, line + dy, dx:dx + 2 * breadth, :])
    linear = jnp.dot(patches[...].astype(jnp.bfloat16), cw[...], preferred_element_type=jnp.float32) + cb[...][None, :]
    level = lax.rsqrt(jnp.mean(linear * linear, -1, keepdims=True) + 1e-06)
    gated = linear * level * ng[...][None, :]
    feat[...] = (gated / (1.0 + jnp.exp(-gated))).astype(feat.dtype)
    feat_out = pltpu.make_async_copy(feat, feat_ref, out_sem.at[1])
    feat_out.start()
    for copy, goes, comes in sends:
        @pl.when(goes)
        def _():
            copy().wait_send()
    out.wait()
    feat_out.wait()


def transformer_part(queries, attn_keys, attn_values, residual, out_weight, out_gate,
                     head_shift, head_scale, head_weight, head_bias, conv_weight, conv_bias, norm_gain):
    nx, nz = lax.axis_size("head"), lax.axis_size("seq") // 2
    frames, height, breadth, features = queries.shape
    model = residual.shape[3]
    rows, width = frames * height * breadth, features // nx
    heads = width // HEAD_DIM
    count = rows * nx
    planes = rows * nz
    share_cols = out_weight.shape[1]
    if nz != 2 * nx or heads != 3:
        raise ValueError("unsupported mesh")
    cells = head_weight.shape[1]
    taps, outs = conv_weight.size // conv_weight.shape[-1], conv_weight.shape[-1]
    places = 4 * rows
    if frames != 2 or conv_weight.shape[:3] != (3, 3, 3) or height != 1:
        raise ValueError("unsupported shape")
    there = pl.BlockSpec(memory_space=pltpu.HBM)
    dma = pltpu.SemaphoreType.DMA
    bf, f32 = jnp.bfloat16, jnp.float32
    tile = 4 * share_cols
    return pl.pallas_call(
        functools.partial(block_kernel, nx, nz, frames),
        out_shape=(jax.ShapeDtypeStruct((rows, model), bf), jax.ShapeDtypeStruct((places, outs), bf)),
        in_specs=[there] * 13,
        out_specs=(there, there),
        scratch_shapes=[
            pltpu.VMEM((count, HEAD_DIM), bf),
            pltpu.VMEM((2, nz, count, HEAD_DIM), bf),
            pltpu.VMEM((2, nz, count, HEAD_DIM), bf),
            pltpu.VMEM((planes, HEAD_DIM), bf),
            pltpu.VMEM((2, nx, planes, HEAD_DIM), bf),
            pltpu.VMEM((2, nx, planes, HEAD_DIM), bf),
            pltpu.VMEM((nz, 2, share_cols, width), bf),
            pltpu.VMEM((heads, HEAD_DIM, count), bf),
            pltpu.VMEM((heads, HEAD_DIM, count), f32),
            pltpu.VMEM((heads, 2, 1, count), f32),
            pltpu.VMEM((count, model), f32),
            pltpu.VMEM((nz // 2 * (nx - 1), rows, tile), bf),
            pltpu.VMEM((nz // 2 * (nx - 1), rows, tile), bf),
            pltpu.VMEM((count, width), bf),
            pltpu.VMEM((planes, HEAD_DIM), bf),
            pltpu.VMEM((rows, model), bf),
            pltpu.VMEM((places, outs), bf),
            pltpu.VMEM((2, 3, rows, 2 * cells), bf),
            pltpu.VMEM((2 * frames, 4, 2 * breadth + 8, cells // 4), f32),
            pltpu.VMEM((places, taps), f32),
            pltpu.VMEM((rows, model), bf),
            pltpu.VMEM((1, model), f32),
            pltpu.VMEM((1, model), f32),
            pltpu.VMEM((1, model), f32),
            pltpu.VMEM((cells, model), bf),
            pltpu.VMEM((1, cells), f32),
            pltpu.VMEM((taps, outs), bf),
            pltpu.VMEM((outs,), f32),
            pltpu.VMEM((outs,), f32),
            dma((16,)), dma((6,)), dma((6,)),
            dma((2,)), dma((4, nz // 2)), dma((2,)), dma((2, nz)),
            dma((2,)), dma((4, nx // 2)), dma((2,)), dma((2, nx)),
            dma((1,)), dma((2 * nx,)),
            dma((1,)), dma((2, nz // 2)), dma((1,)), dma((nz,)),
            dma((1,)), dma((nz // 2 * (nx - 1),)),
            dma((5,)), dma((5,)), dma((2,)),
        ],
        compiler_params=pltpu.CompilerParams(
            collective_id=0, has_side_effects=True, vmem_limit_bytes=56 * 2**20),
        cost_estimate=pl.CostEstimate(flops=4 * count * count * 2 * nz * width, bytes_accessed=2**21, transcendentals=0),
        name="block_ring",
    )(queries.reshape(rows, features), attn_keys.reshape(rows, features), attn_values.reshape(rows, features),
      out_weight.T, residual.reshape(rows, model), out_gate.reshape(1, model), head_shift.reshape(1, model),
      head_scale.reshape(1, model), head_weight.T, head_bias.reshape(1, cells),
      conv_weight.reshape(taps, outs), conv_bias, norm_gain)


def deliver_kernel(a_ref, b_ref, a_out, b_out, sem):
    copies = [pltpu.make_async_copy(a_ref, a_out, sem.at[0]), pltpu.make_async_copy(b_ref, b_out, sem.at[1])]
    for copy in copies:
        copy.start()
    for copy in copies:
        copy.wait()


def deliver(a, b):
    return pl.pallas_call(
        deliver_kernel,
        out_shape=(jax.ShapeDtypeStruct(a.shape, a.dtype), jax.ShapeDtypeStruct(b.shape, b.dtype)),
        in_specs=[pl.BlockSpec(memory_space=pltpu.VMEM)] * 2,
        out_specs=[pl.BlockSpec(memory_space=pltpu.HBM)] * 2,
        scratch_shapes=[pltpu.SemaphoreType.DMA((2,))],
        name="deliver",
    )(a, b)


def on_device(queries, attn_keys, attn_values, residual, out_weight, out_gate, head_shift, head_scale,
              head_weight, head_bias, conv_weight, conv_bias, norm_gain):
    frames, height, breadth = queries.shape[:3]
    hidden, features = transformer_part(queries, attn_keys, attn_values, residual, out_weight, out_gate, head_shift,
                                        head_scale, head_weight, head_bias, conv_weight, conv_bias, norm_gain)
    hidden, features = deliver(hidden, features)
    return hidden.reshape(residual.shape), features.reshape(frames, 2 * height, 2 * breadth, -1)


def solution(mesh):
    return jax.shard_map(
        on_device,
        mesh=mesh,
        in_specs=(
            P(("clip", "head"), "seq", None, None),
            P(("clip", "head"), "seq", None, None),
            P(("clip", "head"), "seq", None, None),
            P(("clip", "head"), "seq", None, None),
            P("head", "seq"),
            P(),
            P(),
            P(),
            P(),
            P(),
            P(),
            P(),
            P(),
        ),
        out_specs=(P(("clip", "head"), "seq", None, None), P(("clip", "head"), "seq", None, None)),
        check_vma=False,
    )
```
